32 devices in a mesh: rows: 32 (over z, y, x, core).
Axes of the slice: x: 2, y: 2, z: 4, core: 2. Of those that a mesh axis runs over, the one named last changes fastest.
Arguments:
- blocks: float32 [512, 4, 256, 256], P('rows'), may hold values from -0.125 to 0.125
- block_cols: int32 [512, 4], P('rows'), may hold values from 0 to 511, as said below
- live_counts: int32 [512], P('rows'), may hold values from 1 to 4, as said below
- onsite_energy: float32 [131072], P('rows'), may hold values from -2 to 2
- precond: float32 [512, 256, 256], P('rows')
- vectors: float32 [32, 131072], P(None, 'rows'), may hold values from -6 to 6
- prev_vectors: float32 [32, 131072], P(None, 'rows'), may hold values from -6 to 6
- prev_image: float32 [32, 131072], P(None, 'rows'), may hold values from -6 to 6
Outputs:
- correction: float32 [32, 131072], P(None, 'rows')
- reduced: float32 [96, 96], replicated
The draws below stay inside these ranges and needn't reach their ends.
Inputs may be any that keep to these rules, and one draw needn't show every extreme that they name: block_cols[b, s] = (b + o) mod 512, with the offsets o of one block-row distinct and within 0 to 4; every slot holds a valid block-column. Slots s < live_counts[b] are live, the rest are ignored; some block-row has 4 live slots in every draw.
All inputs are finite; a program needn't handle non-finite values.
Results may differ from the reference program's by a relative error of at most 0.00026.
Values sent between devices are 32-bit elements; how exact they have to be, the bound alone decides.
A program may use at most 128 MiB of HBM per device.

```python
import jax
import jax.numpy as jnp
from jax import lax

BS = 256
K = 32
BR_DEV = 16
HB = 4
MAXB = 4
ITERS = 3
NBR = 512
NROWS = 131072
BASIS = 96


def draw_block_cols(key, part):
    scores = jax.random.randint(key, (NBR, HB + 1), 0, 1 << 20) * (HB + 1) + jnp.arange(HB + 1, dtype=jnp.int32)[None, :]
    offsets = jnp.argsort(scores, axis=1)[:, :MAXB].astype(jnp.int32)
    return ((jnp.arange(NBR, dtype=jnp.int32)[:, None] + offsets) % NBR).astype(jnp.int32)


def draw_live_counts(key, part):
    first_key = jax.random.fold_in(key, 11)
    second_key = jax.random.fold_in(key, 23)
    third_key = jax.random.fold_in(key, 37)
    shifts = jax.random.randint(first_key, (NBR // BR_DEV,), 0, 3)
    ceiling = jnp.maximum(jnp.right_shift(jnp.full((NBR // BR_DEV,), MAXB, jnp.int32), shifts), 1)
    ceiling_rows = jnp.repeat(ceiling, BR_DEV)
    uniform_ints = jax.random.randint(second_key, (NBR,), 0, 1024)
    counts = 1 + uniform_ints * ceiling_rows // 1024
    position = jax.random.randint(third_key, (), 0, NBR)
    return counts.at[position].set(MAXB).astype(jnp.int32)


def draw_precond(key, part):
    noise = jax.random.normal(key, (NBR, BS, BS), jnp.float32)
    return jnp.eye(BS, dtype=jnp.float32)[None, :, :] + 0.5 * noise / jnp.sqrt(jnp.float32(BS))


def level_of(own_key, extent, shards, least, largest):
    def one(dim, shards_of):
        steps = jax.random.uniform(jax.random.fold_in(jax.random.fold_in(own_key, 6), dim), (shards_of,), jnp.float32, least / len(shards), largest / len(shards))
        return jnp.repeat(jnp.exp(steps), extent[dim] // shards_of).reshape((-1,) + (1,) * (len(extent) - dim - 1))

    loudness = one(*shards[0])
    for cut in shards[1:]:
        loudness = loudness * one(*cut)
    return loudness


def normal_values(key, extent, scale, reach, split=(), kind=jnp.bfloat16):
    drawn = scale * jax.random.normal(key, extent, jnp.float32)
    if split:
        drawn = drawn * level_of(key, extent, split, -0.22, 0.18)
    return jnp.clip(drawn, -reach, reach).astype(kind)


def setup_inputs(seed: int = 0) -> dict:
    seeds = jax.random.split(jax.random.key(seed), 9)
    return {
        "blocks": normal_values(seeds[0], (NBR, MAXB, BS, BS), (2 * MAXB * BS) ** -0.5, 0.125, ((0, 32),), jnp.float32),
        "block_cols": draw_block_cols(jax.random.fold_in(seeds[8], 71), 0),
        "live_counts": draw_live_counts(jax.random.fold_in(seeds[8], 71), 0),
        "onsite_energy": jnp.clip(jax.random.uniform(seeds[3], (NROWS,), jnp.float32, -2.0, 2.0) * level_of(seeds[3], (NROWS,), ((0, 32),), -0.4, 0.0), -2.0, 2.0),
        "precond": draw_precond(jax.random.fold_in(seeds[8], 71), 0),
        "vectors": normal_values(seeds[5], (K, NROWS), 1.0, 6.0, ((1, 32),), jnp.float32),
        "prev_vectors": normal_values(seeds[6], (K, NROWS), 1.0, 6.0, ((1, 32),), jnp.float32),
        "prev_image": normal_values(seeds[7], (K, NROWS), 1.0, 6.0, ((1, 32),), jnp.float32),
    }


def operate(field, blocks, block_cols, live_mask, onsite_energy):
    vec_count = field.shape[0]
    source = field.reshape(vec_count, NBR, BS)
    picked = source[:, block_cols] * live_mask[None, :, :, None]
    forward_part = jnp.einsum('bsij,kbsj->kbi', blocks, picked, precision=lax.Precision.HIGHEST)
    moved = jnp.einsum('kbi,bsij->kbsj', source, blocks, precision=lax.Precision.HIGHEST) * live_mask[None, :, :, None]
    spread = jnp.zeros_like(source).at[:, block_cols].add(moved)
    return onsite_energy[None, :] * field + (forward_part + spread).reshape(vec_count, -1)

def reference(blocks, block_cols, live_counts, onsite_energy, precond, vectors, prev_vectors, prev_image):
    live_mask = (jnp.arange(MAXB, dtype=jnp.int32)[None, :] < live_counts[:, None]).astype(jnp.float32)
    image = operate(vectors, blocks, block_cols, live_mask, onsite_energy)
    quotient = jnp.sum(vectors * image, axis=1) / jnp.sum(vectors * vectors, axis=1)
    remainder = -(image - quotient[:, None] * vectors)
    correction = jnp.zeros_like(vectors)
    hcorr = jnp.zeros_like(vectors)
    for iteration in range(ITERS):
        search = jnp.einsum('bij,kbj->kbi', precond, remainder.reshape(K, NBR, BS), precision=lax.Precision.HIGHEST).reshape(K, -1)
        applied = operate(search, blocks, block_cols, live_mask, onsite_energy) - quotient[:, None] * search
        step_size = jnp.sum(applied * remainder, axis=1) / (jnp.sum(applied * applied, axis=1) + 1.0)
        correction = correction + step_size[:, None] * search
        hcorr = hcorr + step_size[:, None] * (applied + quotient[:, None] * search)
        remainder = remainder - step_size[:, None] * applied
    basis = jnp.concatenate([vectors, prev_vectors, correction], axis=0)
    himage = jnp.concatenate([image, prev_image, hcorr], axis=0)
    gram_matrix = jnp.dot(basis, basis.T, precision=lax.Precision.HIGHEST) + jnp.eye(BASIS, dtype=jnp.float32)
    projected = jnp.dot(basis, himage.T, precision=lax.Precision.HIGHEST)
    factor = jnp.linalg.cholesky(gram_matrix)
    half_way = jax.scipy.linalg.solve_triangular(factor, projected, lower=True)
    reduced = jax.scipy.linalg.solve_triangular(factor, half_way.T, lower=True).T
    return (correction, reduced)
```

```python
import functools

import jax
import jax.numpy as jnp
from jax import lax
from jax.experimental import pallas as pl
from jax.experimental.pallas import tpu as pltpu
from jax.sharding import PartitionSpec as P

HB = 4
MESH = pl.DeviceIdType.MESH
F32 = jnp.float32
BF16 = jnp.bfloat16
E4M3 = jnp.float8_e4m3fn
NN = (((1,), (0,)), ((), ()))
NT = (((1,), (1,)), ((), ()))
LOW = 2.0 ** 20
RING = 8
ROUNDS = 3


def dot(a, b, dims):
    return lax.dot_general(a, b, dims, preferred_element_type=F32)


def hdot(a, b, dims):
    return lax.dot_general(a, b, dims, precision=lax.Precision.HIGHEST, preferred_element_type=F32)


def split(x):
    high = x.astype(BF16)
    low = (x - high.astype(F32)).astype(BF16)
    return high, low


def factor_inverse(s):
    m = s.shape[0]
    rows = lax.broadcasted_iota(jnp.int32, (m, 128), 0)
    lanes = lax.broadcasted_iota(jnp.int32, (m, m), 1)
    eye = jnp.where(lanes == lax.broadcasted_iota(jnp.int32, (m, m), 0), 1.0, 0.0).astype(F32)
    work = jnp.concatenate([s, eye, jnp.zeros((m, 128 - 2 * m), F32)], axis=1)
    diagonal = jnp.ones((m, 128), F32)
    for first in range(0, m, 8):
        column = [jnp.broadcast_to(work[:, first + i:first + i + 1], (m, 128)) for i in range(8)]
        for i in range(8):
            j = first + i
            pivot = column[i][j:j + 1]
            diagonal = jnp.where(rows == j, column[i], diagonal)
            below = jnp.where(rows > j, column[i] * (1.0 / pivot), 0.0)
            work = work - below * work[j:j + 1]
            for k in range(i + 1, 8):
                column[k] = column[k] - below * column[k][j:j + 1]
    return (work / jnp.sqrt(diagonal))[:, m:2 * m]


def kernel(
    n, cols, counts, blocks, precond, onsite_hbm, vectors_hbm, prev_vectors_hbm, prev_image_hbm,
    correction, reduced,
    w_high, w_low, t_high, t_low, m_high, m_low, stage, pstage,
    onsite, vec, pvec, pimg, cor,
    field, fieldv, pair, pairv, moved, movedv, fwd, fwdv,
    image, rem, app, hcorr, srch,
    halo_in, halov_in, land_out, land_in, landv_out, landv_in,
    part, sums_in, e_part, e_in, e_sum, e_all, l_part, l_in, l_sum, l_all, early,
    load_sem, pload_sem, in_sem, out_sem, halo_send, halo_recv, land_send, land_recv,
    sum_send, sum_recv, r_send, r_recv, a_send, a_recv,
):
    me = lax.axis_index("rows")
    right, left = lax.rem(me + 1, n), lax.rem(me + n - 1, n)
    br, slots, bs = blocks.shape[0], blocks.shape[1], blocks.shape[2]
    kv = 32
    total = br * n
    first = br - HB
    order = list(range(first, br)) + list(range(first))
    pchunk = br // 4

    def lanes(b):
        return pl.ds(b * bs, bs)

    def load(t):
        return pltpu.make_async_copy(blocks.at[order[t]], stage.at[t % RING], load_sem.at[t])

    def pload(c):
        at = pl.ds(c * pchunk, pchunk)
        return pltpu.make_async_copy(precond.at[at], pstage.at[at], pload_sem.at[c])

    inputs = [
        pltpu.make_async_copy(vectors_hbm, vec, in_sem.at[0]),
        pltpu.make_async_copy(onsite_hbm, onsite, in_sem.at[1]),
        pltpu.make_async_copy(prev_vectors_hbm, pvec, in_sem.at[2]),
        pltpu.make_async_copy(prev_image_hbm, pimg, in_sem.at[3]),
    ]
    barrier = pltpu.get_barrier_semaphore()
    inputs[0].start()
    inputs[1].start()
    for t in range(RING):
        load(t).start()

    def greet(d, _):
        pl.semaphore_signal(barrier, inc=1, device_id=(lax.rem(me + d, n),), device_id_type=MESH)
        return 0

    lax.fori_loop(1, n, greet, 0)

    def offset(b, s):
        return lax.rem(cols[s, b] - (me * br + b) + total, total)

    def source(b, s):
        return jnp.where(s < counts[b], b + offset(b, s), br + HB)

    def slot_of(b, k):
        at = jnp.int32(slots)
        for s in range(slots):
            at = jnp.where((s < counts[b]) & (offset(b, s) == k), s, at)
        return at

    def put(to, b, x):
        high = x.astype(BF16)
        wide = high.astype(F32)
        to[b, 0:kv] = high
        to[b, kv:2 * kv] = (x - wide).astype(BF16)
        to[b, 2 * kv:3 * kv] = (wide * (1.0 / LOW)).astype(BF16)

    def take_tiles(t):
        b = order[t]
        for s in range(slots):
            at = slice(s * bs, (s + 1) * bs)
            x = stage[t % RING, s]
            high = x.astype(BF16)
            low = ((x - high.astype(F32)) * LOW).astype(E4M3)
            w_high[b, :, at] = high
            w_low[b, :, at] = low
            t_high[b, at, :] = high.T
            t_low[b, at, :] = low.T

    def spread(b, groups):
        lhs = jnp.concatenate([g[0][b, 0:2 * kv] for g in groups], axis=0)
        out = dot(lhs, w_high[b], NN)
        low = dot(jnp.concatenate([g[0][b, 2 * kv:3 * kv] for g in groups], axis=0), w_low[b], NN)
        for i, g in enumerate(groups):
            whole = out[2 * i * kv:(2 * i + 1) * kv] + out[(2 * i + 1) * kv:(2 * i + 2) * kv] + low[i * kv:(i + 1) * kv]
            for s in range(slots):
                g[1][b, s] = whole[:, s * bs:(s + 1) * bs]

    def forward(b, groups):
        at = [source(b, s) for s in range(slots)]
        lhs = jnp.concatenate(
            [jnp.concatenate([g[0][a, 0:2 * kv] for a in at], axis=1) for g in groups], axis=0)
        lhs_low = jnp.concatenate(
            [jnp.concatenate([g[0][a, 2 * kv:3 * kv] for a in at], axis=1) for g in groups], axis=0)
        out = dot(lhs, t_high[b], NN)
        low = dot(lhs_low, t_low[b], NN)
        for i, g in enumerate(groups):
            g[2][b] = out[2 * i * kv:(2 * i + 1) * kv] + out[(2 * i + 1) * kv:(2 * i + 2) * kv] + low[i * kv:(i + 1) * kv]

    def landing(group, b):
        got = None
        for k in range(HB + 1):
            c = b - k
            if 0 <= c < br:
                one = group[1][c, slot_of(c, k)]
                got = one if got is None else got + one
        return got

    def halo_copy(k, src, dst):
        return pltpu.make_async_remote_copy(
            src_ref=src.at[pl.ds(0, HB)], dst_ref=dst,
            send_sem=halo_send.at[k], recv_sem=halo_recv.at[k],
            device_id=(left,), device_id_type=MESH)

    def land_copy(k, src, dst):
        return pltpu.make_async_remote_copy(
            src_ref=src, dst_ref=dst,
            send_sem=land_send.at[k], recv_sem=land_recv.at[k],
            device_id=(right,), device_id_type=MESH)

    main = (pair, moved, fwd)
    side = (pairv, movedv, fwdv)

    def blockloop(lo, hi, body, unroll):
        def step(b, _):
            body(b)
            return 0

        lax.fori_loop(lo, hi, step, 0, unroll=unroll)

    def precondition(b, x):
        high, low = split(x)
        both = dot(jnp.concatenate([high, low], axis=0), m_high[b], NN)
        return both[:kv] + both[kv:] + dot(high, m_low[b], NN)

    def sum_copy(k, d):
        return pltpu.make_async_remote_copy(
            src_ref=part.at[k], dst_ref=sums_in.at[k, me],
            send_sem=sum_send.at[k], recv_sem=sum_recv.at[k],
            device_id=(lax.rem(me + d, n),), device_id_type=MESH)

    def lane_sums(one, two):
        folded = jnp.concatenate([one, two], axis=0)
        folded = folded[:, :128] + folded[:, 128:]
        return jnp.sum(folded, axis=1, keepdims=True)

    def sum_start(k, one, two):
        wide = jnp.broadcast_to(lane_sums(one, two), (2 * kv, 128))
        wide = jnp.concatenate([wide, jnp.zeros((128 - 2 * kv, 128), F32)], axis=0)
        mine = wide.T[:1]
        part[k] = mine
        sums_in[k, me] = mine

        def send(d, _):
            sum_copy(k, d).start()
            return 0

        lax.fori_loop(1, n, send, 0)

    def bulk(ref, sem):
        return pltpu.make_async_copy(ref, ref, sem)

    def sum_finish(k):
        bulk(sums_in.at[k, pl.ds(0, n - 1)], sum_recv.at[k]).wait()
        whole = jnp.sum(sums_in[k], axis=0)
        bulk(sums_in.at[k, pl.ds(0, n - 1)], sum_send.at[k]).wait()
        column = jnp.broadcast_to(whole, (128, 128)).T
        column = jnp.concatenate([column, column], axis=1)
        return column[:kv], column[kv:2 * kv]

    def scatter(r, sheet, held, landed):
        chunks = held.shape[0]
        for c in range(chunks):
            held[c] = sheet[c]

        def send(d, _):
            to = lax.rem(me + d, n)

            @pl.when(to < chunks)
            def _():
                pltpu.make_async_remote_copy(
                    src_ref=held.at[jnp.minimum(to, chunks - 1)], dst_ref=landed.at[me],
                    send_sem=r_send.at[r], recv_sem=r_recv.at[r],
                    device_id=(to,), device_id_type=MESH).start()
            return 0

        lax.fori_loop(1, n, send, 0)

    def spread_sums(r, held, landed, mine, everything):
        chunks = held.shape[0]

        @pl.when(me < chunks)
        def _():
            bulk(landed.at[pl.ds(0, n - 1)], r_recv.at[r]).wait()
            landed[me] = held[jnp.minimum(me, chunks - 1)]
            whole = jnp.sum(landed[...], axis=0)
            mine[...] = whole
            everything[jnp.minimum(me, chunks - 1)] = whole

            def send(d, _):
                pltpu.make_async_remote_copy(
                    src_ref=mine, dst_ref=everything.at[jnp.minimum(me, chunks - 1)],
                    send_sem=a_send.at[r], recv_sem=a_recv.at[r],
                    device_id=(lax.rem(me + d, n),), device_id_type=MESH).start()
                return 0

            lax.fori_loop(1, n, send, 0)

    def collect(r, held, landed, everything):
        chunks = held.shape[0]

        @pl.when(me < chunks)
        def _():
            bulk(everything.at[pl.ds(0, chunks - 1)], a_recv.at[r]).wait()

        @pl.when(me >= chunks)
        def _():
            bulk(everything, a_recv.at[r]).wait()

    def drain(r, held, landed):
        chunks = held.shape[0]

        @pl.when(me < chunks)
        def _():
            bulk(held.at[pl.ds(0, chunks - 1)], r_send.at[r]).wait()
            bulk(landed.at[pl.ds(0, n - 1)], a_send.at[r]).wait()

        @pl.when(me >= chunks)
        def _():
            bulk(held, r_send.at[r]).wait()

    zero = jnp.zeros((kv, bs), F32)
    for c in range(br):
        moved[c, slots] = zero
        movedv[c, slots] = zero
    pair[br + HB] = jnp.zeros((3 * kv, bs), BF16)
    pairv[br + HB] = jnp.zeros((3 * kv, bs), BF16)
    inputs[0].wait()
    for b in range(br):
        x = vec[:, lanes(b)]
        put(pair, b, x)
        if b < HB:
            field[b] = x

    def advance(t):
        load(t).wait()
        take_tiles(t)
        if t + RING < br:
            load(t + RING).start()
        elif t + RING == br:
            for c in range(4):
                pload(c).start()
            inputs[2].start()
            inputs[3].start()

    for t in range(HB):
        advance(t)
        spread(order[t], [main])
    for i in range(HB):
        land_out[i] = landing(main, br + i)
    pl.semaphore_wait(barrier, n - 1)
    halo = halo_copy(0, field, halo_in.at[0])
    halo.start()
    land = land_copy(0, land_out, land_in.at[0])
    land.start()
    for t in range(HB, br):
        advance(t)
        spread(order[t], [main])
        if t - HB >= HB:
            forward(t - 2 * HB, [main])
    for b in range(first - HB, first):
        forward(b, [main])

    for c in range(4):
        pload(c).wait()
    for b in range(br):
        high, low = split(pstage[b])
        m_high[b] = high.T
        m_low[b] = low.T

    def side_block(b):
        x = precondition(b, vec[:, lanes(b)])
        fieldv[b] = x
        put(pairv, b, x)

    for b in list(range(HB)) + list(range(first, br)):
        side_block(b)
    halov = halo_copy(4, fieldv, halov_in)
    halov.start()
    for b in range(first, br):
        spread(b, [side])
    for i in range(HB):
        landv_out[i] = landing(side, br + i)
    landv = land_copy(4, landv_out, landv_in)
    landv.start()
    for b in range(HB, first):
        side_block(b)

    inputs[1].wait()

    def finish(k, groups, halo, land, more):
        halo.wait_recv()
        for i in range(HB):
            put(pair, br + i, halo_in[k, i])
        if more:
            more[0].wait_recv()
            for i in range(HB):
                put(pairv, br + i, halov_in[i])
        for b in range(first, br):
            forward(b, groups)
        land.wait_recv()
        if more:
            more[1].wait_recv()
        for copy in (halo, land) + tuple(more):
            copy.wait_send()

    def applied(k, group, landed, held, b):
        got = group[2][b] + landing(group, b) + onsite[:, lanes(b)] * held[b]
        return got + landed(b) if b < HB else got

    def middle(k, update, groups):
        sums = [zero, zero]

        def one(b):
            out, a, c = update(b)
            sums[0] = sums[0] + a
            sums[1] = sums[1] + c
            return out

        def pre(b, x):
            y = precondition(b, x)
            field[b] = y
            put(pair, b, y)

        for b in range(HB):
            pre(b, one(b))
        halo = halo_copy(k, field, halo_in.at[k])
        halo.start()
        outs = [one(b) for b in range(first, br)]
        for b in range(first, br):
            pre(b, outs[b - first])
        for b in range(first, br):
            spread(b, [main])
        for i in range(HB):
            land_out[i] = landing(main, br + i)
        land = land_copy(k, land_out, land_in.at[k])
        land.start()
        outs = [one(b) for b in range(HB, first)]
        sum_start(k - 1, *sums)
        for b in range(HB, first):
            pre(b, outs[b - HB])
        blockloop(0, first, lambda b: spread(b, groups), 4)
        blockloop(0, first, lambda b: forward(b, groups), 4)
        return halo, land

    finish(0, [main], halo, land, ())

    def after0(b):
        x = vec[:, lanes(b)]
        got = fwd[b] + landing(main, b) + onsite[:, lanes(b)] * x
        if b < HB:
            got = got + land_in[0, b]
        image[b] = got
        return got, x * got, x * x

    halo, land = middle(1, after0, [main, side])
    inputs[2].wait()
    inputs[3].wait()
    both = jnp.zeros((2 * kv, 4 * kv), F32)
    for b in range(br):
        basis = jnp.concatenate([vec[:, lanes(b)], pvec[:, lanes(b)]], axis=0)
        other = jnp.concatenate([basis, image[b], pimg[:, lanes(b)]], axis=0)
        oh, ol = split(other)
        bh, bl = oh[:2 * kv], ol[:2 * kv]
        both = both + dot(bh, oh, NT) + dot(bl, oh, NT) + dot(bh, ol, NT)
    scatter(0, [both[c * 8:(c + 1) * 8] for c in range(8)], e_part, e_in)
    finish(1, [main, side], halo, land, (halov, landv))
    numerator, denominator = sum_finish(0)
    quotient = numerator / denominator

    def after1(b):
        xv, xi = fieldv[b], field[b]
        on = onsite[:, lanes(b)]
        hv = fwdv[b] + landing(side, b) + on * xv
        hi = fwd[b] + landing(main, b) + on * xi
        if b < HB:
            hv = hv + landv_in[b]
            hi = hi + land_in[1, b]
        x = quotient * xv - xi
        r = quotient * vec[:, lanes(b)] - image[b]
        a = quotient * hv - hi - quotient * x
        srch[b] = x
        rem[b] = r
        app[b] = a
        return a, a * r, a * a

    halo, land = middle(2, after1, [main])
    spread_sums(0, e_part, e_in, e_sum, e_all)
    finish(2, [main], halo, land, ())
    step = sum_finish(1)
    step = step[0] / (step[1] + 1.0)

    def advance_step(k, start, b):
        x, y, t = srch[b], app[b], field[b]
        on = onsite[:, lanes(b)]
        g = fwd[b] + landing(main, b) + (on - quotient) * t
        if b < HB:
            g = g + land_in[k, b]
        c = step * x
        h = step * (y + quotient * x)
        cor[:, lanes(b)] = c if start else cor[:, lanes(b)] + c
        hcorr[b] = h if start else hcorr[b] + h
        r = rem[b] - step * y
        z = y - step * g
        srch[b] = x - step * t
        rem[b] = r
        app[b] = z
        return z, z * r, z * z

    halo, land = middle(3, lambda b: advance_step(2, True, b), [main])
    collect(0, e_part, e_in, e_all)
    known = jnp.concatenate([e_all[c] for c in range(8)], axis=0)
    rows_at = lax.broadcasted_iota(jnp.int32, (kv, kv), 0)
    eye = jnp.where(rows_at == lax.broadcasted_iota(jnp.int32, (kv, kv), 1), 1.0, 0.0).astype(F32)
    x11 = factor_inverse(known[:kv, :kv] + eye)
    y21 = hdot(known[kv:2 * kv, :kv], x11, NT)
    x22 = factor_inverse(known[kv:2 * kv, kv:2 * kv] + eye - hdot(y21, y21, NT))
    x21 = -hdot(x22, hdot(y21, x11, NN), NN)
    early[0:kv] = jnp.concatenate([x11, jnp.zeros((kv, 128 - kv), F32)], axis=1)
    early[kv:2 * kv] = jnp.concatenate([x21, x22, jnp.zeros((kv, 128 - 2 * kv), F32)], axis=1)
    finish(3, [main], halo, land, ())
    step = sum_finish(2)
    step = step[0] / (step[1] + 1.0)

    sums = [zero, zero]
    both = jnp.zeros((4 * kv, 8 * kv), F32)
    for b in range(br):
        z, one, two = advance_step(3, False, b)
        sums = [sums[0] + one, sums[1] + two]
        x = srch[b]
        mine = cor[:, lanes(b)]
        hmine = hcorr[b]
        w = z + quotient * x
        ch, cl = split(jnp.concatenate([mine, x], axis=0))
        hh, hl = split(jnp.concatenate([hmine, w], axis=0))
        vh, vl = split(jnp.concatenate([vec[:, lanes(b)], pvec[:, lanes(b)]], axis=0))
        ih, il = split(jnp.concatenate([image[b], pimg[:, lanes(b)]], axis=0))
        lh = jnp.concatenate([ch, hh], axis=0)
        ll = jnp.concatenate([cl, hl], axis=0)
        oh = jnp.concatenate([vh, ch, ih, hh], axis=0)
        ol = jnp.concatenate([vl, cl, il, hl], axis=0)
        both = both + dot(lh, oh, NT) + dot(ll, oh, NT) + dot(lh, ol, NT)
    lane_at = lax.broadcasted_iota(jnp.int32, (2 * kv, 128), 1)
    third = jnp.where(
        lane_at < 2 * kv, both[2 * kv:, :128], jnp.broadcast_to(lane_sums(*sums), (2 * kv, 128)))
    sheets = [both[:2 * kv, :128], both[:2 * kv, 128:], third]
    scatter(1, [s[c * 8:(c + 1) * 8] for s in sheets for c in range(8)], l_part, l_in)
    spread_sums(1, l_part, l_in, l_sum, l_all)
    collect(1, l_part, l_in, l_all)
    one, two, three = [
        jnp.concatenate([l_all[8 * i + c] for c in range(8)], axis=0) for i in range(3)]
    cross = jnp.broadcast_to(three[:kv, 2 * kv:2 * kv + 1], (kv, 128))
    own = jnp.broadcast_to(three[kv:, 2 * kv:2 * kv + 1], (kv, 128))
    step = cross / (own + 1.0)
    wide = jnp.concatenate([step, step], axis=1)
    for b in range(br):
        cor[:, lanes(b)] = cor[:, lanes(b)] + wide * srch[b]
    result = pltpu.make_async_copy(cor, correction, out_sem.at[0])
    result.start()
    row = jnp.concatenate([step, jnp.zeros((128 - kv, 128), F32)], axis=0).T[:kv, :kv]
    one = one[:kv] + step * one[kv:]
    two = two[:kv] + step * two[kv:]
    three = three[:kv] + step * three[kv:]
    gc = one[:, :2 * kv]
    gcc = one[:, 2 * kv:3 * kv] + one[:, 3 * kv:] * row
    pc = two[:, :2 * kv]
    pcc = two[:, 2 * kv:3 * kv] + two[:, 3 * kv:] * row
    pe = jnp.concatenate([e_all[c] for c in range(8)], axis=0)[:, 2 * kv:]
    pec = jnp.concatenate([three, jnp.zeros((128 - kv, 128), F32)], axis=0).T[:2 * kv, :kv]
    xe = early[:, :2 * kv]
    y = hdot(gc, xe, NT)
    xc = factor_inverse(gcc + eye - hdot(y, y, NT))
    xl = -hdot(xc, hdot(y, xe, NN), NN)
    x = jnp.concatenate([
        jnp.concatenate([xe, jnp.zeros((2 * kv, kv), F32)], axis=1),
        jnp.concatenate([xl, xc], axis=1)], axis=0)
    p = jnp.concatenate([
        jnp.concatenate([pe, pec], axis=1),
        jnp.concatenate([pc, pcc], axis=1)], axis=0)
    reduced[...] = hdot(hdot(x, p, NN), x, NT)
    drain(0, e_part, e_in)
    drain(1, l_part, l_in)
    result.wait()


def local(blocks, block_cols, live_counts, onsite_energy, precond, vectors, prev_vectors, prev_image):
    n = lax.axis_size("rows")
    br, slots, bs, _ = blocks.shape
    kv, width = vectors.shape
    nb = 3 * kv
    vmem = pl.BlockSpec(memory_space=pltpu.VMEM)
    smem = pl.BlockSpec(memory_space=pltpu.SMEM)
    hbm = pl.BlockSpec(memory_space=pl.ANY)
    dma = pltpu.SemaphoreType.DMA
    field = pltpu.VMEM((br, kv, bs), F32)
    halo = pltpu.VMEM((HB, kv, bs), F32)
    pair = pltpu.VMEM((br + HB + 1, 3 * kv, bs), BF16)
    moved = pltpu.VMEM((br, slots + 1, kv, bs), F32)
    return pl.pallas_call(
        functools.partial(kernel, n),
        out_shape=(
            jax.ShapeDtypeStruct((kv, width), F32),
            jax.ShapeDtypeStruct((nb, nb), F32),
        ),
        in_specs=[smem, smem, hbm, hbm, hbm, hbm, hbm, hbm],
        out_specs=(hbm, vmem),
        scratch_shapes=[
            pltpu.VMEM((br, bs, slots * bs), BF16),
            pltpu.VMEM((br, bs, slots * bs), E4M3),
            pltpu.VMEM((br, slots * bs, bs), BF16),
            pltpu.VMEM((br, slots * bs, bs), E4M3),
            pltpu.VMEM((br, bs, bs), BF16),
            pltpu.VMEM((br, bs, bs), BF16),
            pltpu.VMEM((RING, slots, bs, bs), F32),
            pltpu.VMEM((br, bs, bs), F32),
            pltpu.VMEM((1, width), F32),
            pltpu.VMEM((kv, width), F32),
            pltpu.VMEM((kv, width), F32),
            pltpu.VMEM((kv, width), F32),
            pltpu.VMEM((kv, width), F32),
            field, field, pair, pair, moved, moved, field, field,
            field, field, field, field, field,
            pltpu.VMEM((4, HB, kv, bs), F32),
            halo, halo,
            pltpu.VMEM((4, HB, kv, bs), F32),
            halo, halo,
            pltpu.VMEM((ROUNDS, 1, 128), F32),
            pltpu.VMEM((ROUNDS, n, 1, 128), F32),
            pltpu.VMEM((8, 8, 128), F32),
            pltpu.VMEM((n, 8, 128), F32),
            pltpu.VMEM((8, 128), F32),
            pltpu.VMEM((8, 8, 128), F32),
            pltpu.VMEM((24, 8, 128), F32),
            pltpu.VMEM((n, 8, 128), F32),
            pltpu.VMEM((8, 128), F32),
            pltpu.VMEM((24, 8, 128), F32),
            pltpu.VMEM((2 * kv, 128), F32),
            dma((br,)),
            dma((4,)),
            dma((4,)),
            dma((1,)),
            dma((5,)),
            dma((5,)),
            dma((5,)),
            dma((5,)),
            dma((ROUNDS,)),
            dma((ROUNDS,)),
            dma((2,)),
            dma((2,)),
            dma((2,)),
            dma((2,)),
        ],
        compiler_params=pltpu.CompilerParams(
            collective_id=0, has_side_effects=True, vmem_limit_bytes=67043328
        ),
    )(block_cols.T, live_counts, blocks, precond, onsite_energy[None, :], vectors, prev_vectors, prev_image)


def solution(mesh):
    placed = (
        P("rows", None, None, None),
        P("rows", None),
        P("rows"),
        P("rows"),
        P("rows", None, None),
        P(None, "rows"),
        P(None, "rows"),
        P(None, "rows"),
    )
    return jax.shard_map(
        local, mesh=mesh, in_specs=placed, out_specs=(P(None, "rows"), P()), check_vma=False
    )
```

```python
import functools

import jax
import jax.numpy as jnp
from jax import lax
from jax.experimental import pallas as pl
from jax.experimental.pallas import tpu as pltpu
from jax.sharding import PartitionSpec as P

HB = 4
MESH = pl.DeviceIdType.MESH
F32 = jnp.float32
BF16 = jnp.bfloat16
E4M3 = jnp.float8_e4m3fn
NN = (((1,), (0,)), ((), ()))
NT = (((1,), (1,)), ((), ()))
LOW = 2.0 ** 20
RING = 8
ROUNDS = 3


def dot(a, b, dims):
    return lax.dot_general(a, b, dims, preferred_element_type=F32)


def hdot(a, b, dims):
    return lax.dot_general(a, b, dims, precision=lax.Precision.HIGHEST, preferred_element_type=F32)


def split(x):
    high = x.astype(BF16)
    low = (x - high.astype(F32)).astype(BF16)
    return high, low


def factor_inverse(s):
    m = s.shape[0]
    rows = lax.broadcasted_iota(jnp.int32, (m, 128), 0)
    lanes = lax.broadcasted_iota(jnp.int32, (m, m), 1)
    eye = jnp.where(lanes == lax.broadcasted_iota(jnp.int32, (m, m), 0), 1.0, 0.0).astype(F32)
    work = jnp.concatenate([s, eye, jnp.zeros((m, 128 - 2 * m), F32)], axis=1)
    diagonal = jnp.ones((m, 128), F32)
    for first in range(0, m, 8):
        column = [jnp.broadcast_to(work[:, first + i:first + i + 1], (m, 128)) for i in range(8)]
        for i in range(8):
            j = first + i
            pivot = column[i][j:j + 1]
            diagonal = jnp.where(rows == j, column[i], diagonal)
            below = jnp.where(rows > j, column[i] * (1.0 / pivot), 0.0)
            work = work - below * work[j:j + 1]
            for k in range(i + 1, 8):
                column[k] = column[k] - below * column[k][j:j + 1]
    return (work / jnp.sqrt(diagonal))[:, m:2 * m]


def kernel(
    n, cols, counts, blocks, precond, onsite_hbm, vectors_hbm, prev_vectors_hbm, prev_image_hbm,
    correction, reduced,
    w_high, w_low, t_high, t_low, m_high, m_low, stage, pstage,
    onsite, vec, pvec, pimg, cor,
    field, fieldv, pair, pairv, pairp, moved, movedv, movedp, fwd, fwdv, fwdp,
    image, rem, app, srch, hsrch, hturn,
    halo_in, halov_in, land_out, land_in, landv_out, landv_in, p_out, p_in, landp_out, landp_in,
    part, sums_in, x_part, x_in, x_sum, x_all, y_part, y_in, y_sum, y_all,
    f_part, f_in, early,
    load_sem, pload_sem, in_sem, out_sem, halo_send, halo_recv, land_send, land_recv,
    sum_send, sum_recv, r_send, r_recv, a_send, a_recv, f_send, f_recv,
):
    me = lax.axis_index("rows")
    right, left = lax.rem(me + 1, n), lax.rem(me + n - 1, n)
    br, slots, bs = blocks.shape[0], blocks.shape[1], blocks.shape[2]
    kv = 32
    total = br * n
    first = br - HB
    order = list(range(first, br)) + list(range(first))
    pchunk = br // 4

    def lanes(b):
        return pl.ds(b * bs, bs)

    def load(t):
        return pltpu.make_async_copy(blocks.at[order[t]], stage.at[t % RING], load_sem.at[t])

    def pload(c):
        at = pl.ds(c * pchunk, pchunk)
        return pltpu.make_async_copy(precond.at[at], pstage.at[at], pload_sem.at[c])

    inputs = [
        pltpu.make_async_copy(vectors_hbm, vec, in_sem.at[0]),
        pltpu.make_async_copy(onsite_hbm, onsite, in_sem.at[1]),
        pltpu.make_async_copy(prev_vectors_hbm, pvec, in_sem.at[2]),
        pltpu.make_async_copy(prev_image_hbm, pimg, in_sem.at[3]),
    ]
    barrier = pltpu.get_barrier_semaphore()
    inputs[0].start()
    inputs[1].start()
    for t in range(RING):
        load(t).start()

    def greet(d, _):
        pl.semaphore_signal(barrier, inc=1, device_id=(lax.rem(me + d, n),), device_id_type=MESH)
        return 0

    lax.fori_loop(1, n, greet, 0)

    def offset(b, s):
        return lax.rem(cols[s, b] - (me * br + b) + total, total)

    def source(b, s):
        return jnp.where(s < counts[b], b + offset(b, s), br + HB)

    def slot_of(b, k):
        at = jnp.int32(slots)
        for s in range(slots):
            at = jnp.where((s < counts[b]) & (offset(b, s) == k), s, at)
        return at

    def put(to, b, x):
        high = x.astype(BF16)
        wide = high.astype(F32)
        to[b, 0:kv] = high
        to[b, kv:2 * kv] = (x - wide).astype(BF16)
        to[b, 2 * kv:3 * kv] = (wide * (1.0 / LOW)).astype(BF16)

    def take_tiles(t):
        b = order[t]
        for s in range(slots):
            at = slice(s * bs, (s + 1) * bs)
            x = stage[t % RING, s]
            high = x.astype(BF16)
            low = ((x - high.astype(F32)) * LOW).astype(E4M3)
            w_high[b, :, at] = high
            w_low[b, :, at] = low
            t_high[b, at, :] = high.T
            t_low[b, at, :] = low.T

    def spread(b, groups):
        lhs = jnp.concatenate([g[0][b, 0:2 * kv] for g in groups], axis=0)
        out = dot(lhs, w_high[b], NN)
        low = dot(jnp.concatenate([g[0][b, 2 * kv:3 * kv] for g in groups], axis=0), w_low[b], NN)
        for i, g in enumerate(groups):
            whole = out[2 * i * kv:(2 * i + 1) * kv] + out[(2 * i + 1) * kv:(2 * i + 2) * kv] + low[i * kv:(i + 1) * kv]
            for s in range(slots):
                g[1][b, s] = whole[:, s * bs:(s + 1) * bs]

    def forward(b, groups):
        at = [source(b, s) for s in range(slots)]
        lhs = jnp.concatenate(
            [jnp.concatenate([g[0][a, 0:2 * kv] for a in at], axis=1) for g in groups], axis=0)
        lhs_low = jnp.concatenate(
            [jnp.concatenate([g[0][a, 2 * kv:3 * kv] for a in at], axis=1) for g in groups], axis=0)
        out = dot(lhs, t_high[b], NN)
        low = dot(lhs_low, t_low[b], NN)
        for i, g in enumerate(groups):
            g[2][b] = out[2 * i * kv:(2 * i + 1) * kv] + out[(2 * i + 1) * kv:(2 * i + 2) * kv] + low[i * kv:(i + 1) * kv]

    def landing(group, b):
        got = None
        for k in range(HB + 1):
            c = b - k
            if 0 <= c < br:
                one = group[1][c, slot_of(c, k)]
                got = one if got is None else got + one
        return got

    def halo_copy(k, src, dst):
        return pltpu.make_async_remote_copy(
            src_ref=src.at[pl.ds(0, HB)], dst_ref=dst,
            send_sem=halo_send.at[k], recv_sem=halo_recv.at[k],
            device_id=(left,), device_id_type=MESH)

    def land_copy(k, src, dst):
        return pltpu.make_async_remote_copy(
            src_ref=src, dst_ref=dst,
            send_sem=land_send.at[k], recv_sem=land_recv.at[k],
            device_id=(right,), device_id_type=MESH)

    main = (pair, moved, fwd)
    side = (pairv, movedv, fwdv)
    rear = (pairp, movedp, fwdp)

    def blockloop(lo, hi, body, unroll):
        def step(b, _):
            body(b)
            return 0

        lax.fori_loop(lo, hi, step, 0, unroll=unroll)

    def precondition(b, x):
        high, low = split(x)
        both = dot(jnp.concatenate([high, low], axis=0), m_high[b], NN)
        return both[:kv] + both[kv:] + dot(high, m_low[b], NN)

    def every(lo, hi, body):
        if hi - lo <= 32:
            for d in range(lo, hi):
                body(d)
        else:
            def step(d, _):
                body(d)
                return 0

            lax.fori_loop(lo, hi, step, 0)

    def sum_copy(k, d):
        return pltpu.make_async_remote_copy(
            src_ref=part.at[k], dst_ref=sums_in.at[k, me],
            send_sem=sum_send.at[k], recv_sem=sum_recv.at[k],
            device_id=(lax.rem(me + d, n),), device_id_type=MESH)

    def lane_sums(one, two):
        folded = jnp.concatenate([one, two], axis=0)
        folded = folded[:, :128] + folded[:, 128:]
        return jnp.sum(folded, axis=1, keepdims=True)

    def sum_start(k, one, two):
        wide = jnp.broadcast_to(lane_sums(one, two), (2 * kv, 128))
        wide = jnp.concatenate([wide, jnp.zeros((128 - 2 * kv, 128), F32)], axis=0)
        mine = wide.T[:1]
        part[k] = mine
        sums_in[k, me] = mine

        every(1, n, lambda d: sum_copy(k, d).start())

    def bulk(ref, sem):
        return pltpu.make_async_copy(ref, ref, sem)

    def sum_finish(k):
        bulk(sums_in.at[k, pl.ds(0, n - 1)], sum_recv.at[k]).wait()
        whole = jnp.sum(sums_in[k], axis=0)
        bulk(sums_in.at[k, pl.ds(0, n - 1)], sum_send.at[k]).wait()
        column = jnp.broadcast_to(whole, (128, 128)).T
        column = jnp.concatenate([column, column], axis=1)
        return column[:kv], column[kv:2 * kv]

    def scatter(r, sheet, held, landed):
        chunks = held.shape[0]
        for c in range(chunks):
            if sheet[c] is not None:
                held[c] = sheet[c]

        def send(d):
            to = lax.rem(me + d, chunks)

            @pl.when(to != me)
            def _():
                pltpu.make_async_remote_copy(
                    src_ref=held.at[to], dst_ref=landed.at[me],
                    send_sem=r_send.at[r], recv_sem=r_recv.at[r],
                    device_id=(to,), device_id_type=MESH).start()

        every(0, chunks, send)

    def spread_sums(r, held, landed, mine, everything):
        chunks = held.shape[0]

        @pl.when(me < chunks)
        def _():
            bulk(landed.at[pl.ds(0, n - 1)], r_recv.at[r]).wait()
            landed[me] = held[jnp.minimum(me, chunks - 1)]
            whole = jnp.sum(landed[...], axis=0)
            mine[...] = whole
            everything[jnp.minimum(me, chunks - 1)] = whole

            def send(d):
                pltpu.make_async_remote_copy(
                    src_ref=mine, dst_ref=everything.at[jnp.minimum(me, chunks - 1)],
                    send_sem=a_send.at[r], recv_sem=a_recv.at[r],
                    device_id=(lax.rem(me + d, n),), device_id_type=MESH).start()

            every(1, n, send)

    def collect(r, held, landed, everything):
        chunks = held.shape[0]

        @pl.when(me < chunks)
        def _():
            bulk(everything.at[pl.ds(0, chunks - 1)], a_recv.at[r]).wait()

        @pl.when(me >= chunks)
        def _():
            bulk(everything, a_recv.at[r]).wait()

    def drain(r, held, landed):
        chunks = held.shape[0]

        @pl.when(me < chunks)
        def _():
            bulk(held.at[pl.ds(0, chunks - 1)], r_send.at[r]).wait()
            bulk(landed.at[pl.ds(0, n - 1)], a_send.at[r]).wait()

        @pl.when(me >= chunks)
        def _():
            bulk(held, r_send.at[r]).wait()

    zero = jnp.zeros((kv, bs), F32)
    for c in range(br):
        moved[c, slots] = zero
        movedv[c, slots] = zero
        movedp[c, slots] = zero
    pair[br + HB] = jnp.zeros((3 * kv, bs), BF16)
    pairv[br + HB] = jnp.zeros((3 * kv, bs), BF16)
    pairp[br + HB] = jnp.zeros((3 * kv, bs), BF16)
    inputs[0].wait()
    for b in range(br):
        x = vec[:, lanes(b)]
        put(pair, b, x)
        if b < HB:
            field[b] = x

    def advance(t):
        load(t).wait()
        take_tiles(t)
        if t + RING < br:
            load(t + RING).start()
        elif t + RING == br:
            for c in range(4):
                pload(c).start()
            inputs[2].start()
            inputs[3].start()

    for t in range(HB):
        advance(t)
        spread(order[t], [main])
    for i in range(HB):
        land_out[i] = landing(main, br + i)
    pl.semaphore_wait(barrier, n - 1)
    halo = halo_copy(0, field, halo_in.at[0])
    halo.start()
    land = land_copy(0, land_out, land_in.at[0])
    land.start()
    for t in range(HB, br):
        advance(t)
        spread(order[t], [main])
        if t - HB >= HB:
            forward(t - 2 * HB, [main])
    for b in range(first - HB, first):
        forward(b, [main])

    for c in range(4):
        pload(c).wait()
    for b in range(br):
        high, low = split(pstage[b])
        m_high[b] = high.T
        m_low[b] = low.T

    def side_block(b):
        x = precondition(b, vec[:, lanes(b)])
        fieldv[b] = x
        put(pairv, b, x)

    for b in list(range(HB)) + list(range(first, br)):
        side_block(b)
    halov = halo_copy(4, fieldv, halov_in)
    halov.start()
    for b in range(first, br):
        spread(b, [side])
    for i in range(HB):
        landv_out[i] = landing(side, br + i)
    landv = land_copy(4, landv_out, landv_in)
    landv.start()
    for b in range(HB, first):
        side_block(b)

    inputs[1].wait()

    def finish(k, groups, halo, land, more):
        halo.wait_recv()
        for i in range(HB):
            put(pair, br + i, halo_in[k, i])
        for group, copies, arrived in more:
            copies[0].wait_recv()
            for i in range(HB):
                put(group[0], br + i, arrived[i])
        for b in range(first, br):
            forward(b, groups)
        land.wait_recv()
        for group, copies, arrived in more:
            copies[1].wait_recv()
            copies[0].wait_send()
            copies[1].wait_send()
        halo.wait_send()
        land.wait_send()

    def begin(k, update, outs_to, groups):
        def pre(b, x):
            y = precondition(b, x)
            outs_to[b] = y
            put(pair, b, y)

        for b in range(HB):
            pre(b, update(b))
        halo = halo_copy(k, outs_to, halo_in.at[k])
        halo.start()
        outs = [update(b) for b in range(first, br)]
        for b in range(first, br):
            pre(b, outs[b - first])
        for b in range(first, br):
            spread(b, [main])
        for i in range(HB):
            land_out[i] = landing(main, br + i)
        land = land_copy(k, land_out, land_in.at[k])
        land.start()
        outs = [update(b) for b in range(HB, first)]

        def rest():
            for b in range(HB, first):
                pre(b, outs[b - HB])

        return halo, land, rest

    def middle(groups):
        def both_ways(b):
            spread(b, groups)
            forward(b, groups)

        blockloop(0, first, both_ways, 4)

    def totals():
        sums = [zero, zero]

        def add(a, c):
            sums[0] = sums[0] + a
            sums[1] = sums[1] + c

        return sums, add

    def gram(lhs, rhs):
        got = None
        for b in range(br):
            lh, ll = split(jnp.concatenate(lhs(b), axis=0))
            rh, rl = split(jnp.concatenate(rhs(b), axis=0))
            m = lh.shape[0]
            both = dot(jnp.concatenate([lh, ll], axis=0), rh, NT)
            one = both[:m] + both[m:] + dot(lh, rl, NT)
            got = one if got is None else got + one
        return got

    def rows8(sheets):
        return [s[c * 8:(c + 1) * 8] for s in sheets for c in range(s.shape[0] // 8)]

    finish(0, [main], halo, land, ())

    sums, add = totals()

    def after0(b):
        x = vec[:, lanes(b)]
        got = fwd[b] + landing(main, b) + onsite[:, lanes(b)] * x
        if b < HB:
            got = got + land_in[0, b]
        image[b] = got
        add(x * got, x * x)
        return got

    halo, land, rest = begin(1, after0, field, [main])
    sum_start(0, *sums)
    rest()
    middle([main, side])
    inputs[2].wait()
    inputs[3].wait()
    for b in range(br):
        x = pvec[:, lanes(b)]
        put(pairp, b, x)
        if b < HB:
            p_out[b] = x
    halop = halo_copy(5, p_out, p_in)
    halop.start()
    for b in range(first, br):
        spread(b, [rear])
    for i in range(HB):
        landp_out[i] = landing(rear, br + i)
    landp = land_copy(5, landp_out, landp_in)
    landp.start()
    both = gram(lambda b: [vec[:, lanes(b)], pvec[:, lanes(b)]],
                lambda b: [vec[:, lanes(b)], pvec[:, lanes(b)], image[b], pimg[:, lanes(b)]])
    for c, rows in enumerate(rows8([both])):
        x_part[c] = rows
    finish(1, [main, side], halo, land, [(side, (halov, landv), halov_in)])
    numerator, denominator = sum_finish(0)
    quotient = numerator / denominator

    sums, add = totals()

    def after1(b):
        xv, xi = fieldv[b], field[b]
        on = onsite[:, lanes(b)]
        hv = fwdv[b] + landing(side, b) + on * xv
        hi = fwd[b] + landing(main, b) + on * xi
        if b < HB:
            hv = hv + landv_in[b]
            hi = hi + land_in[1, b]
        x = quotient * xv - xi
        h = quotient * hv - hi
        r = quotient * vec[:, lanes(b)] - image[b]
        a = h - quotient * x
        srch[b] = x
        hsrch[b] = h
        rem[b] = r
        app[b] = a
        add(a * r, a * a)
        return a

    halo, land, rest = begin(2, after1, field, [main])
    sum_start(1, *sums)
    rest()
    middle([main, rear])
    both = gram(lambda b: [srch[b], field[b]],
                lambda b: [vec[:, lanes(b)], pvec[:, lanes(b)], srch[b], field[b],
                           image[b], pimg[:, lanes(b)], hsrch[b], hsrch[b]])
    scatter(0, [None] * 8 + rows8([both[:, :128], both[:, 128:]]), x_part, x_in)
    finish(2, [main, rear], halo, land, [(rear, (halop, landp), p_in)])

    def after2(b):
        t = field[b]
        got = fwd[b] + landing(main, b) + onsite[:, lanes(b)] * t
        if b < HB:
            got = got + land_in[2, b]
        hturn[b] = got
        return got - quotient * t

    halo, land, rest = begin(3, after2, fieldv, [main])
    step = sum_finish(1)
    step1 = step[0] / (step[1] + 1.0)
    sums, add = totals()
    for b in range(br):
        r = rem[b] - step1 * app[b]
        a = app[b] - step1 * (hturn[b] - quotient * field[b])
        rem[b] = r
        app[b] = a
        add(a * r, a * a)
    sum_start(2, *sums)
    rest()
    for b in range(br):
        got = fwdp[b] + landing(rear, b) + onsite[:, lanes(b)] * pvec[:, lanes(b)]
        fwdp[b] = got + landp_in[b] if b < HB else got
    one = gram(lambda b: [fieldv[b]],
               lambda b: [vec[:, lanes(b)], pvec[:, lanes(b)], srch[b], field[b],
                          image[b], pimg[:, lanes(b)], hsrch[b], fieldv[b]])
    two = gram(lambda b: [fieldv[b], srch[b], field[b]], lambda b: [fwdp[b], hturn[b]])
    three = jnp.concatenate([two[:kv], two[2 * kv:]], axis=1)
    four = jnp.concatenate([two[kv:2 * kv], two[kv:2 * kv]], axis=1)
    scatter(1, rows8([one[:, :128], one[:, 128:], three, four]), y_part, y_in)
    middle([main])
    spread_sums(0, x_part, x_in, x_sum, x_all)
    finish(3, [main], halo, land, ())
    step = sum_finish(2)
    step2 = step[0] / (step[1] + 1.0)

    sums, add = totals()
    for b in range(br):
        u = fieldv[b]
        got = fwd[b] + landing(main, b) + onsite[:, lanes(b)] * u
        if b < HB:
            got = got + land_in[3, b]
        image[b] = got
        a = app[b]
        r = rem[b] - step2 * a
        g = hturn[b] - quotient * field[b]
        a = a - step2 * (g - step1 * (got - quotient * u))
        add(a * r, a * a)
    square = gram(lambda b: [fieldv[b]], lambda b: [image[b]])
    flat = jnp.concatenate([square[8 * c:8 * c + 8] for c in range(4)], axis=1)
    wide = jnp.broadcast_to(lane_sums(*sums), (2 * kv, 128))
    wide = jnp.concatenate([wide, jnp.zeros((128 - 2 * kv, 128), F32)], axis=0)
    f_part[8] = wide.T[:1]
    for i in range(8):
        f_part[i] = flat[i:i + 1]
    f_in[me] = f_part[...]

    def last_send(d):
        pltpu.make_async_remote_copy(
            src_ref=f_part, dst_ref=f_in.at[me],
            send_sem=f_send.at[0], recv_sem=f_recv.at[0],
            device_id=(lax.rem(me + d, n),), device_id_type=MESH).start()

    every(1, n, last_send)

    spread_sums(1, y_part, y_in, y_sum, y_all)

    collect(0, x_part, x_in, x_all)
    known = jnp.concatenate([x_all[c] for c in range(8)], axis=0)
    rows_at = lax.broadcasted_iota(jnp.int32, (kv, kv), 0)
    eye = jnp.where(rows_at == lax.broadcasted_iota(jnp.int32, (kv, kv), 1), 1.0, 0.0).astype(F32)
    x11 = factor_inverse(known[:kv, :kv] + eye)
    y21 = hdot(known[kv:2 * kv, :kv], x11, NT)
    x22 = factor_inverse(known[kv:2 * kv, kv:2 * kv] + eye - hdot(y21, y21, NT))
    x21 = -hdot(x22, hdot(y21, x11, NN), NN)
    early[0:kv] = jnp.concatenate([x11, jnp.zeros((kv, 128 - kv), F32)], axis=1)
    early[kv:2 * kv] = jnp.concatenate([x21, x22, jnp.zeros((kv, 128 - 2 * kv), F32)], axis=1)
    collect(1, y_part, y_in, y_all)

    def sheet(held, i, count):
        return jnp.concatenate([held[i * count + c] for c in range(count)], axis=0)

    def turned(t):
        return jnp.concatenate([t, jnp.zeros((128 - kv, 128), F32)], axis=0).T[:, :kv]

    xg, xh = sheet(x_all, 1, 8), sheet(x_all, 2, 8)
    ug, uh, third, fourth = [sheet(y_all, i, 4) for i in range(4)]
    ug_t, uh_t, third_t = turned(ug), turned(uh), turned(third)
    bulk(f_in.at[pl.ds(0, n - 1)], f_recv.at[0]).wait()
    whole = jnp.sum(f_in[...], axis=0)
    bulk(f_in.at[pl.ds(0, n - 1)], f_send.at[0]).wait()
    flat = jnp.concatenate([whole[i] for i in range(8)], axis=0)
    uhu = jnp.concatenate([flat[:, kv * c:kv * c + kv] for c in range(4)], axis=0)
    column = jnp.broadcast_to(whole[8], (128, 128)).T
    step3 = column[:kv] / (column[kv:2 * kv] + 1.0)
    step1, step2 = step1[:, :128], step2[:, :128]
    ca = step1 + step2 + step3
    ct = -(step1 * step2 + step3 * (step1 + step2))
    cu = step1 * step2 * step3
    wa, wt, wu = [jnp.concatenate([c, c], axis=1) for c in (ca, ct, cu)]
    for b in range(br):
        cor[:, lanes(b)] = wa * srch[b] + wt * field[b] + wu * fieldv[b]
    result = pltpu.make_async_copy(cor, correction, out_sem.at[0])
    result.start()
    row = jnp.concatenate([ca, ct, cu, jnp.zeros((128 - 3 * kv, 128), F32)], axis=0).T
    ra, rt, ru = [row[:kv, kv * i:kv * i + kv] for i in range(3)]
    g = ca * xg[:kv] + ct * xg[kv:] + cu * ug
    h = ca * xh[:kv] + ct * xh[kv:] + cu * uh
    na, nt, nu = ca[:, :kv], ct[:, :kv], cu[:, :kv]
    gu = na * ug_t[2 * kv:3 * kv] + nt * ug_t[3 * kv:] + nu * uh[:, 3 * kv:]
    gc = g[:, :2 * kv]
    gcc = g[:, 2 * kv:3 * kv] * ra + g[:, 3 * kv:] * rt + gu * ru
    pc = h[:, :2 * kv]
    both = ca * jnp.concatenate([fourth[:, :2 * kv], fourth[:, :2 * kv]], axis=1) + cu * third
    chp = both[:, :kv] + nt * third[:, 2 * kv:3 * kv]
    cht = both[:, kv:2 * kv] + nt * third[:, 3 * kv:]
    chu = na * uh_t[2 * kv:3 * kv] + nt * third_t[kv:2 * kv] + nu * uhu
    pcc = h[:, 2 * kv:3 * kv] * ra + cht * rt + chu * ru
    pec = turned(jnp.concatenate([h[:, :kv], chp, jnp.zeros((kv, 128 - 2 * kv), F32)], axis=1))[:2 * kv]
    pe = sheet(x_all, 0, 8)[:, 2 * kv:]
    xe = early[:, :2 * kv]
    y = hdot(gc, xe, NT)
    xc = factor_inverse(gcc + eye - hdot(y, y, NT))
    xl = -hdot(xc, hdot(y, xe, NN), NN)
    x = jnp.concatenate([
        jnp.concatenate([xe, jnp.zeros((2 * kv, kv), F32)], axis=1),
        jnp.concatenate([xl, xc], axis=1)], axis=0)
    p = jnp.concatenate([
        jnp.concatenate([pe, pec], axis=1),
        jnp.concatenate([pc, pcc], axis=1)], axis=0)
    reduced[...] = hdot(hdot(x, p, NN), x, NT)
    drain(0, x_part, x_in)
    drain(1, y_part, y_in)
    result.wait()


def local(blocks, block_cols, live_counts, onsite_energy, precond, vectors, prev_vectors, prev_image):
    n = lax.axis_size("rows")
    br, slots, bs, _ = blocks.shape
    kv, width = vectors.shape
    nb = 3 * kv
    vmem = pl.BlockSpec(memory_space=pltpu.VMEM)
    smem = pl.BlockSpec(memory_space=pltpu.SMEM)
    hbm = pl.BlockSpec(memory_space=pl.ANY)
    dma = pltpu.SemaphoreType.DMA
    field = pltpu.VMEM((br, kv, bs), F32)
    halo = pltpu.VMEM((HB, kv, bs), F32)
    pair = pltpu.VMEM((br + HB + 1, 3 * kv, bs), BF16)
    moved = pltpu.VMEM((br, slots + 1, kv, bs), F32)

    def reduction(chunks):
        tiles = [(chunks, 8, 128), (n, 8, 128), (8, 128), (chunks, 8, 128)]
        return [pltpu.VMEM(t, F32) for t in tiles]

    return pl.pallas_call(
        functools.partial(kernel, n),
        out_shape=(
            jax.ShapeDtypeStruct((kv, width), F32),
            jax.ShapeDtypeStruct((nb, nb), F32),
        ),
        in_specs=[smem, smem, hbm, hbm, hbm, hbm, hbm, hbm],
        out_specs=(hbm, vmem),
        scratch_shapes=[
            pltpu.VMEM((br, bs, slots * bs), BF16),
            pltpu.VMEM((br, bs, slots * bs), E4M3),
            pltpu.VMEM((br, slots * bs, bs), BF16),
            pltpu.VMEM((br, slots * bs, bs), E4M3),
            pltpu.VMEM((br, bs, bs), BF16),
            pltpu.VMEM((br, bs, bs), BF16),
            pltpu.VMEM((RING, slots, bs, bs), F32),
            pltpu.VMEM((br, bs, bs), F32),
            pltpu.VMEM((1, width), F32),
            pltpu.VMEM((kv, width), F32),
            pltpu.VMEM((kv, width), F32),
            pltpu.VMEM((kv, width), F32),
            pltpu.VMEM((kv, width), F32),
            field, field, pair, pair, pair, moved, moved, moved, field, field, field,
            field, field, field, field, field, field,
            pltpu.VMEM((4, HB, kv, bs), F32),
            halo, halo,
            pltpu.VMEM((4, HB, kv, bs), F32),
            halo, halo, halo, halo, halo, halo,
            pltpu.VMEM((ROUNDS, 1, 128), F32),
            pltpu.VMEM((ROUNDS, n, 1, 128), F32),
            *reduction(24), *reduction(16),
            pltpu.VMEM((9, 1, 128), F32),
            pltpu.VMEM((n, 9, 1, 128), F32),
            pltpu.VMEM((2 * kv, 128), F32),
            dma((br,)),
            dma((4,)),
            dma((4,)),
            dma((1,)),
            dma((6,)),
            dma((6,)),
            dma((6,)),
            dma((6,)),
            dma((ROUNDS,)),
            dma((ROUNDS,)),
            dma((2,)),
            dma((2,)),
            dma((2,)),
            dma((2,)),
            dma((1,)),
            dma((1,)),
        ],
        compiler_params=pltpu.CompilerParams(
            collective_id=0, has_side_effects=True, vmem_limit_bytes=67043328
        ),
    )(block_cols.T, live_counts, blocks, precond, onsite_energy[None, :], vectors, prev_vectors, prev_image)


def solution(mesh):
    placed = (
        P("rows", None, None, None),
        P("rows", None),
        P("rows"),
        P("rows"),
        P("rows", None, None),
        P(None, "rows"),
        P(None, "rows"),
        P(None, "rows"),
    )
    return jax.shard_map(
        local, mesh=mesh, in_specs=placed, out_specs=(P(None, "rows"), P()), check_vma=False
    )
```

```python
import functools

import jax
import jax.numpy as jnp
from jax import lax
from jax.experimental import pallas as pl
from jax.experimental.pallas import tpu as pltpu
from jax.sharding import PartitionSpec as P

HB = 4
MESH = pl.DeviceIdType.MESH
F32 = jnp.float32
BF16 = jnp.bfloat16
E4M3 = jnp.float8_e4m3fn
NN = (((1,), (0,)), ((), ()))
NT = (((1,), (1,)), ((), ()))
LOW = 2.0 ** 20
RING = 8
ROUNDS = 3


def dot(a, b, dims):
    return lax.dot_general(a, b, dims, preferred_element_type=F32)


def hdot(a, b, dims):
    return lax.dot_general(a, b, dims, precision=lax.Precision.HIGHEST, preferred_element_type=F32)


def split(x):
    high = x.astype(BF16)
    low = (x - high.astype(F32)).astype(BF16)
    return high, low


def factor_inverse(s):
    m = s.shape[0]
    rows = lax.broadcasted_iota(jnp.int32, (m, 128), 0)
    lanes = lax.broadcasted_iota(jnp.int32, (m, m), 1)
    eye = jnp.where(lanes == lax.broadcasted_iota(jnp.int32, (m, m), 0), 1.0, 0.0).astype(F32)
    work = jnp.concatenate([s, eye, jnp.zeros((m, 128 - 2 * m), F32)], axis=1)
    diagonal = jnp.ones((m, 128), F32)
    for first in range(0, m, 8):
        column = [jnp.broadcast_to(work[:, first + i:first + i + 1], (m, 128)) for i in range(8)]
        for i in range(8):
            j = first + i
            pivot = column[i][j:j + 1]
            diagonal = jnp.where(rows == j, column[i], diagonal)
            below = jnp.where(rows > j, column[i] * (1.0 / pivot), 0.0)
            work = work - below * work[j:j + 1]
            for k in range(i + 1, 8):
                column[k] = column[k] - below * column[k][j:j + 1]
    return (work / jnp.sqrt(diagonal))[:, m:2 * m]


def kernel(
    n, cols, counts, blocks, precond, onsite_hbm, vectors_hbm, prev_vectors_hbm, prev_image_hbm,
    correction, reduced,
    w_high, w_low, t_high, t_low, m_high, m_low, stage, pstage,
    onsite, vec, pvec, pimg, cor,
    field, fieldv, pair, pairv, pairp, moved, movedv, movedp, fwd, fwdv, fwdp,
    image, rem, app, srch, hsrch, hturn,
    halo_in, halov_in, land_out, land_in, landv_out, landv_in, p_out, p_in, landp_out, landp_in,
    part, sums_in, x_part, x_in, x_sum, x_all, y_part, y_in, y_sum, y_all,
    f_part, f_in, early,
    load_sem, pload_sem, in_sem, out_sem, halo_send, halo_recv, land_send, land_recv,
    sum_send, sum_recv, r_send, r_recv, a_send, a_recv, f_send, f_recv,
):
    me = lax.axis_index("rows")
    right, left = lax.rem(me + 1, n), lax.rem(me + n - 1, n)
    br, slots, bs = blocks.shape[0], blocks.shape[1], blocks.shape[2]
    kv = 32
    total = br * n
    first = br - HB
    order = list(range(first, br)) + list(range(first))
    pchunk = br // 4

    def lanes(b):
        return pl.ds(b * bs, bs)

    def load(t):
        return pltpu.make_async_copy(blocks.at[order[t]], stage.at[t % RING], load_sem.at[t])

    def pload(c):
        at = pl.ds(c * pchunk, pchunk)
        return pltpu.make_async_copy(precond.at[at], pstage.at[at], pload_sem.at[c])

    inputs = [
        pltpu.make_async_copy(vectors_hbm, vec, in_sem.at[0]),
        pltpu.make_async_copy(onsite_hbm, onsite, in_sem.at[1]),
        pltpu.make_async_copy(prev_vectors_hbm, pvec, in_sem.at[2]),
        pltpu.make_async_copy(prev_image_hbm, pimg, in_sem.at[3]),
    ]
    barrier = pltpu.get_barrier_semaphore()
    inputs[0].start()
    inputs[1].start()
    for t in range(RING):
        load(t).start()
    for c in range(4):
        pload(c).start()
    inputs[2].start()
    inputs[3].start()

    def greet(d, _):
        pl.semaphore_signal(barrier, inc=1, device_id=(lax.rem(me + d, n),), device_id_type=MESH)
        return 0

    lax.fori_loop(1, n, greet, 0)

    def offset(b, s):
        return lax.rem(cols[s, b] - (me * br + b) + total, total)

    def source(b, s):
        return jnp.where(s < counts[b], b + offset(b, s), br + HB)

    def slot_of(b, k):
        at = jnp.int32(slots)
        for s in range(slots):
            at = jnp.where((s < counts[b]) & (offset(b, s) == k), s, at)
        return at

    def put(to, b, x):
        high = x.astype(BF16)
        wide = high.astype(F32)
        to[b, 0:kv] = high
        to[b, kv:2 * kv] = (x - wide).astype(BF16)
        to[b, 2 * kv:3 * kv] = (wide * (1.0 / LOW)).astype(BF16)

    def take_tiles(t):
        b = order[t]
        for s in range(slots):
            at = slice(s * bs, (s + 1) * bs)
            x = stage[t % RING, s]
            high = x.astype(BF16)
            low = ((x - high.astype(F32)) * LOW).astype(E4M3)
            w_high[b, :, at] = high
            w_low[b, :, at] = low
            t_high[b, at, :] = high.T
            t_low[b, at, :] = low.T

    def spread(b, groups):
        lhs = jnp.concatenate([g[0][b, 0:2 * kv] for g in groups], axis=0)
        out = dot(lhs, w_high[b], NN)
        low = dot(jnp.concatenate([g[0][b, 2 * kv:3 * kv] for g in groups], axis=0), w_low[b], NN)
        for i, g in enumerate(groups):
            whole = out[2 * i * kv:(2 * i + 1) * kv] + out[(2 * i + 1) * kv:(2 * i + 2) * kv] + low[i * kv:(i + 1) * kv]
            for s in range(slots):
                g[1][b, s] = whole[:, s * bs:(s + 1) * bs]

    def forward(b, groups):
        at = [source(b, s) for s in range(slots)]
        lhs = jnp.concatenate(
            [jnp.concatenate([g[0][a, 0:2 * kv] for a in at], axis=1) for g in groups], axis=0)
        lhs_low = jnp.concatenate(
            [jnp.concatenate([g[0][a, 2 * kv:3 * kv] for a in at], axis=1) for g in groups], axis=0)
        out = dot(lhs, t_high[b], NN)
        low = dot(lhs_low, t_low[b], NN)
        for i, g in enumerate(groups):
            g[2][b] = out[2 * i * kv:(2 * i + 1) * kv] + out[(2 * i + 1) * kv:(2 * i + 2) * kv] + low[i * kv:(i + 1) * kv]

    def landing(group, b):
        got = None
        for k in range(HB + 1):
            c = b - k
            if 0 <= c < br:
                one = group[1][c, slot_of(c, k)]
                got = one if got is None else got + one
        return got

    def halo_copy(k, src, dst):
        return pltpu.make_async_remote_copy(
            src_ref=src.at[pl.ds(0, HB)], dst_ref=dst,
            send_sem=halo_send.at[k], recv_sem=halo_recv.at[k],
            device_id=(left,), device_id_type=MESH)

    def land_copy(k, src, dst):
        return pltpu.make_async_remote_copy(
            src_ref=src, dst_ref=dst,
            send_sem=land_send.at[k], recv_sem=land_recv.at[k],
            device_id=(right,), device_id_type=MESH)

    main = (pair, moved, fwd)
    side = (pairv, movedv, fwdv)
    rear = (pairp, movedp, fwdp)

    def blockloop(lo, hi, body, unroll):
        def step(b, _):
            body(b)
            return 0

        lax.fori_loop(lo, hi, step, 0, unroll=unroll)

    def precondition(b, x):
        high, low = split(x)
        both = dot(jnp.concatenate([high, low], axis=0), m_high[b], NN)
        return both[:kv] + both[kv:] + dot(high, m_low[b], NN)

    def every(lo, hi, body):
        if hi - lo <= 32:
            for d in range(lo, hi):
                body(d)
        else:
            def step(d, _):
                body(d)
                return 0

            lax.fori_loop(lo, hi, step, 0)

    def sum_copy(k, d):
        return pltpu.make_async_remote_copy(
            src_ref=part.at[k], dst_ref=sums_in.at[k, me],
            send_sem=sum_send.at[k], recv_sem=sum_recv.at[k],
            device_id=(lax.rem(me + d, n),), device_id_type=MESH)

    def lane_sums(one, two):
        folded = jnp.concatenate([one, two], axis=0)
        folded = folded[:, :128] + folded[:, 128:]
        return jnp.sum(folded, axis=1, keepdims=True)

    def sum_start(k, one, two):
        wide = jnp.broadcast_to(lane_sums(one, two), (2 * kv, 128))
        wide = jnp.concatenate([wide, jnp.zeros((128 - 2 * kv, 128), F32)], axis=0)
        mine = wide.T[:1]
        part[k] = mine
        sums_in[k, me] = mine

        every(1, n, lambda d: sum_copy(k, d).start())

    def bulk(ref, sem):
        return pltpu.make_async_copy(ref, ref, sem)

    def sum_finish(k):
        bulk(sums_in.at[k, pl.ds(0, n - 1)], sum_recv.at[k]).wait()
        whole = jnp.sum(sums_in[k], axis=0)
        bulk(sums_in.at[k, pl.ds(0, n - 1)], sum_send.at[k]).wait()
        column = jnp.broadcast_to(whole, (128, 128)).T
        column = jnp.concatenate([column, column], axis=1)
        return column[:kv], column[kv:2 * kv]

    def scatter(r, sheet, held, landed):
        chunks = held.shape[0]
        for c in range(chunks):
            if sheet[c] is not None:
                held[c] = sheet[c]

        def send(d):
            to = lax.rem(me + d, chunks)

            @pl.when(to != me)
            def _():
                pltpu.make_async_remote_copy(
                    src_ref=held.at[to], dst_ref=landed.at[me],
                    send_sem=r_send.at[r], recv_sem=r_recv.at[r],
                    device_id=(to,), device_id_type=MESH).start()

        every(0, chunks, send)

    def spread_sums(r, held, landed, mine, everything):
        chunks = held.shape[0]

        @pl.when(me < chunks)
        def _():
            bulk(landed.at[pl.ds(0, n - 1)], r_recv.at[r]).wait()
            landed[me] = held[jnp.minimum(me, chunks - 1)]
            whole = jnp.sum(landed[...], axis=0)
            mine[...] = whole
            everything[jnp.minimum(me, chunks - 1)] = whole

            def send(d):
                pltpu.make_async_remote_copy(
                    src_ref=mine, dst_ref=everything.at[jnp.minimum(me, chunks - 1)],
                    send_sem=a_send.at[r], recv_sem=a_recv.at[r],
                    device_id=(lax.rem(me + d, n),), device_id_type=MESH).start()

            every(1, n, send)

    def collect(r, held, landed, everything):
        chunks = held.shape[0]

        @pl.when(me < chunks)
        def _():
            bulk(everything.at[pl.ds(0, chunks - 1)], a_recv.at[r]).wait()

        @pl.when(me >= chunks)
        def _():
            bulk(everything, a_recv.at[r]).wait()

    def drain(r, held, landed):
        chunks = held.shape[0]

        @pl.when(me < chunks)
        def _():
            bulk(held.at[pl.ds(0, chunks - 1)], r_send.at[r]).wait()
            bulk(landed.at[pl.ds(0, n - 1)], a_send.at[r]).wait()

        @pl.when(me >= chunks)
        def _():
            bulk(held, r_send.at[r]).wait()

    zero = jnp.zeros((kv, bs), F32)
    for c in range(br):
        moved[c, slots] = zero
        movedv[c, slots] = zero
        movedp[c, slots] = zero
    pair[br + HB] = jnp.zeros((3 * kv, bs), BF16)
    pairv[br + HB] = jnp.zeros((3 * kv, bs), BF16)
    pairp[br + HB] = jnp.zeros((3 * kv, bs), BF16)
    inputs[0].wait()
    for b in range(br):
        x = vec[:, lanes(b)]
        put(pair, b, x)
        if b < HB:
            field[b] = x

    def advance(t):
        load(t).wait()
        if t and t - 1 + RING < br:
            load(t - 1 + RING).start()

    for t in range(HB):
        advance(t)
        if t:
            spread(order[t - 1], [main])
        take_tiles(t)
    spread(order[HB - 1], [main])
    for i in range(HB):
        land_out[i] = landing(main, br + i)
    pl.semaphore_wait(barrier, n - 1)
    halo = halo_copy(0, field, halo_in.at[0])
    halo.start()
    land = land_copy(0, land_out, land_in.at[0])
    land.start()
    for t in range(HB, br):
        advance(t)
        if t > HB:
            spread(order[t - 1], [main])
            forward(order[t - 1], [main])
        take_tiles(t)
    spread(first - 1, [main])
    forward(first - 1, [main])

    for c in range(4):
        pload(c).wait()
    for b in range(br):
        high, low = split(pstage[b])
        m_high[b] = high.T
        m_low[b] = low.T

    def side_block(b):
        x = precondition(b, vec[:, lanes(b)])
        fieldv[b] = x
        put(pairv, b, x)

    for b in list(range(HB)) + list(range(first, br)):
        side_block(b)
    halov = halo_copy(4, fieldv, halov_in)
    halov.start()
    for b in range(first, br):
        spread(b, [side])
    for i in range(HB):
        landv_out[i] = landing(side, br + i)
    landv = land_copy(4, landv_out, landv_in)
    landv.start()
    for b in range(HB, first):
        side_block(b)

    inputs[1].wait()

    def finish(k, groups, halo, land, more):
        halo.wait_recv()
        for i in range(HB):
            put(pair, br + i, halo_in[k, i])
        for group, copies, arrived in more:
            copies[0].wait_recv()
            for i in range(HB):
                put(group[0], br + i, arrived[i])
        for b in range(first, br):
            forward(b, groups)
        land.wait_recv()
        for group, copies, arrived in more:
            copies[1].wait_recv()
            copies[0].wait_send()
            copies[1].wait_send()
        halo.wait_send()
        land.wait_send()

    def begin(k, update, outs_to, groups):
        def pre(b, x):
            y = precondition(b, x)
            outs_to[b] = y
            put(pair, b, y)

        for b in range(HB):
            pre(b, update(b))
        halo = halo_copy(k, outs_to, halo_in.at[k])
        halo.start()
        outs = [update(b) for b in range(first, br)]
        for b in range(first, br):
            pre(b, outs[b - first])
        for b in range(first, br):
            spread(b, [main])
        for i in range(HB):
            land_out[i] = landing(main, br + i)
        land = land_copy(k, land_out, land_in.at[k])
        land.start()
        outs = [update(b) for b in range(HB, first)]

        def rest():
            for b in range(HB, first):
                pre(b, outs[b - HB])

        return halo, land, rest

    def middle(groups):
        def both_ways(b):
            spread(b, groups)
            forward(b, groups)

        blockloop(0, first, both_ways, 4)

    def totals():
        sums = [zero, zero]

        def add(a, c):
            sums[0] = sums[0] + a
            sums[1] = sums[1] + c

        return sums, add

    def gram(lhs, rhs):
        got = None
        for b in range(br):
            lh, ll = split(jnp.concatenate(lhs(b), axis=0))
            rh, rl = split(jnp.concatenate(rhs(b), axis=0))
            m = lh.shape[0]
            both = dot(jnp.concatenate([lh, ll], axis=0), rh, NT)
            one = both[:m] + both[m:] + dot(lh, rl, NT)
            got = one if got is None else got + one
        return got

    def rows8(sheets):
        return [s[c * 8:(c + 1) * 8] for s in sheets for c in range(s.shape[0] // 8)]

    finish(0, [main], halo, land, ())

    sums, add = totals()

    def after0(b):
        x = vec[:, lanes(b)]
        got = fwd[b] + landing(main, b) + onsite[:, lanes(b)] * x
        if b < HB:
            got = got + land_in[0, b]
        image[b] = got
        add(x * got, x * x)
        return got

    halo, land, rest = begin(1, after0, field, [main])
    sum_start(0, *sums)
    rest()
    middle([main, side])
    inputs[2].wait()
    inputs[3].wait()
    for b in range(br):
        x = pvec[:, lanes(b)]
        put(pairp, b, x)
        if b < HB:
            p_out[b] = x
    halop = halo_copy(5, p_out, p_in)
    halop.start()
    for b in range(first, br):
        spread(b, [rear])
    for i in range(HB):
        landp_out[i] = landing(rear, br + i)
    landp = land_copy(5, landp_out, landp_in)
    landp.start()
    both = gram(lambda b: [vec[:, lanes(b)], pvec[:, lanes(b)]],
                lambda b: [vec[:, lanes(b)], pvec[:, lanes(b)], image[b], pimg[:, lanes(b)]])
    for c, rows in enumerate(rows8([both])):
        x_part[c] = rows
    finish(1, [main, side], halo, land, [(side, (halov, landv), halov_in)])
    numerator, denominator = sum_finish(0)
    quotient = numerator / denominator

    sums, add = totals()

    def after1(b):
        xv, xi = fieldv[b], field[b]
        on = onsite[:, lanes(b)]
        hv = fwdv[b] + landing(side, b) + on * xv
        hi = fwd[b] + landing(main, b) + on * xi
        if b < HB:
            hv = hv + landv_in[b]
            hi = hi + land_in[1, b]
        x = quotient * xv - xi
        h = quotient * hv - hi
        r = quotient * vec[:, lanes(b)] - image[b]
        a = h - quotient * x
        srch[b] = x
        hsrch[b] = h
        rem[b] = r
        app[b] = a
        add(a * r, a * a)
        return a

    halo, land, rest = begin(2, after1, field, [main])
    sum_start(1, *sums)
    rest()
    middle([main, rear])
    both = gram(lambda b: [srch[b], field[b]],
                lambda b: [vec[:, lanes(b)], pvec[:, lanes(b)], srch[b], field[b],
                           image[b], pimg[:, lanes(b)], hsrch[b], hsrch[b]])
    scatter(0, [None] * 8 + rows8([both[:, :128], both[:, 128:]]), x_part, x_in)
    finish(2, [main, rear], halo, land, [(rear, (halop, landp), p_in)])

    def after2(b):
        t = field[b]
        got = fwd[b] + landing(main, b) + onsite[:, lanes(b)] * t
        if b < HB:
            got = got + land_in[2, b]
        hturn[b] = got
        return got - quotient * t

    halo, land, rest = begin(3, after2, fieldv, [main])
    step = sum_finish(1)
    step1 = step[0] / (step[1] + 1.0)
    sums, add = totals()
    for b in range(br):
        r = rem[b] - step1 * app[b]
        a = app[b] - step1 * (hturn[b] - quotient * field[b])
        rem[b] = r
        app[b] = a
        add(a * r, a * a)
    sum_start(2, *sums)
    rest()
    for b in range(br):
        got = fwdp[b] + landing(rear, b) + onsite[:, lanes(b)] * pvec[:, lanes(b)]
        fwdp[b] = got + landp_in[b] if b < HB else got
    one = gram(lambda b: [fieldv[b]],
               lambda b: [vec[:, lanes(b)], pvec[:, lanes(b)], srch[b], field[b],
                          image[b], pimg[:, lanes(b)], hsrch[b], fieldv[b]])
    two = gram(lambda b: [fieldv[b], srch[b], field[b]], lambda b: [fwdp[b], hturn[b]])
    three = jnp.concatenate([two[:kv], two[2 * kv:]], axis=1)
    four = jnp.concatenate([two[kv:2 * kv], two[kv:2 * kv]], axis=1)
    scatter(1, rows8([one[:, :128], one[:, 128:], three, four]), y_part, y_in)
    middle([main])
    spread_sums(0, x_part, x_in, x_sum, x_all)
    finish(3, [main], halo, land, ())
    spread_sums(1, y_part, y_in, y_sum, y_all)
    step = sum_finish(2)
    step2 = step[0] / (step[1] + 1.0)

    sums, add = totals()
    for b in range(br):
        u = fieldv[b]
        got = fwd[b] + landing(main, b) + onsite[:, lanes(b)] * u
        if b < HB:
            got = got + land_in[3, b]
        image[b] = got
        a = app[b]
        r = rem[b] - step2 * a
        g = hturn[b] - quotient * field[b]
        a = a - step2 * (g - step1 * (got - quotient * u))
        add(a * r, a * a)
    square = gram(lambda b: [fieldv[b]], lambda b: [image[b]])
    flat = jnp.concatenate([square[8 * c:8 * c + 8] for c in range(4)], axis=1)
    wide = jnp.broadcast_to(lane_sums(*sums), (2 * kv, 128))
    wide = jnp.concatenate([wide, jnp.zeros((128 - 2 * kv, 128), F32)], axis=0)
    f_part[8] = wide.T[:1]
    for i in range(8):
        f_part[i] = flat[i:i + 1]
    f_in[me] = f_part[...]

    def last_send(d):
        pltpu.make_async_remote_copy(
            src_ref=f_part, dst_ref=f_in.at[me],
            send_sem=f_send.at[0], recv_sem=f_recv.at[0],
            device_id=(lax.rem(me + d, n),), device_id_type=MESH).start()

    every(1, n, last_send)


    collect(0, x_part, x_in, x_all)
    known = jnp.concatenate([x_all[c] for c in range(8)], axis=0)
    rows_at = lax.broadcasted_iota(jnp.int32, (kv, kv), 0)
    eye = jnp.where(rows_at == lax.broadcasted_iota(jnp.int32, (kv, kv), 1), 1.0, 0.0).astype(F32)
    x11 = factor_inverse(known[:kv, :kv] + eye)
    y21 = hdot(known[kv:2 * kv, :kv], x11, NT)
    x22 = factor_inverse(known[kv:2 * kv, kv:2 * kv] + eye - hdot(y21, y21, NT))
    x21 = -hdot(x22, hdot(y21, x11, NN), NN)
    early[0:kv] = jnp.concatenate([x11, jnp.zeros((kv, 128 - kv), F32)], axis=1)
    early[kv:2 * kv] = jnp.concatenate([x21, x22, jnp.zeros((kv, 128 - 2 * kv), F32)], axis=1)
    collect(1, y_part, y_in, y_all)

    def sheet(held, i, count):
        return jnp.concatenate([held[i * count + c] for c in range(count)], axis=0)

    def turned(t):
        return jnp.concatenate([t, jnp.zeros((128 - kv, 128), F32)], axis=0).T[:, :kv]

    xg, xh = sheet(x_all, 1, 8), sheet(x_all, 2, 8)
    ug, uh, third, fourth = [sheet(y_all, i, 4) for i in range(4)]
    ug_t, uh_t, third_t = turned(ug), turned(uh), turned(third)
    bulk(f_in.at[pl.ds(0, n - 1)], f_recv.at[0]).wait()
    whole = jnp.sum(f_in[...], axis=0)
    bulk(f_in.at[pl.ds(0, n - 1)], f_send.at[0]).wait()
    flat = jnp.concatenate([whole[i] for i in range(8)], axis=0)
    uhu = jnp.concatenate([flat[:, kv * c:kv * c + kv] for c in range(4)], axis=0)
    column = jnp.broadcast_to(whole[8], (128, 128)).T
    step3 = column[:kv] / (column[kv:2 * kv] + 1.0)
    step1, step2 = step1[:, :128], step2[:, :128]
    ca = step1 + step2 + step3
    ct = -(step1 * step2 + step3 * (step1 + step2))
    cu = step1 * step2 * step3
    wa, wt, wu = [jnp.concatenate([c, c], axis=1) for c in (ca, ct, cu)]
    for b in range(br):
        cor[:, lanes(b)] = wa * srch[b] + wt * field[b] + wu * fieldv[b]
    result = pltpu.make_async_copy(cor, correction, out_sem.at[0])
    result.start()
    row = jnp.concatenate([ca, ct, cu, jnp.zeros((128 - 3 * kv, 128), F32)], axis=0).T
    ra, rt, ru = [row[:kv, kv * i:kv * i + kv] for i in range(3)]
    g = ca * xg[:kv] + ct * xg[kv:] + cu * ug
    h = ca * xh[:kv] + ct * xh[kv:] + cu * uh
    na, nt, nu = ca[:, :kv], ct[:, :kv], cu[:, :kv]
    gu = na * ug_t[2 * kv:3 * kv] + nt * ug_t[3 * kv:] + nu * uh[:, 3 * kv:]
    gc = g[:, :2 * kv]
    gcc = g[:, 2 * kv:3 * kv] * ra + g[:, 3 * kv:] * rt + gu * ru
    pc = h[:, :2 * kv]
    both = ca * jnp.concatenate([fourth[:, :2 * kv], fourth[:, :2 * kv]], axis=1) + cu * third
    chp = both[:, :kv] + nt * third[:, 2 * kv:3 * kv]
    cht = both[:, kv:2 * kv] + nt * third[:, 3 * kv:]
    chu = na * uh_t[2 * kv:3 * kv] + nt * third_t[kv:2 * kv] + nu * uhu
    pcc = h[:, 2 * kv:3 * kv] * ra + cht * rt + chu * ru
    pec = turned(jnp.concatenate([h[:, :kv], chp, jnp.zeros((kv, 128 - 2 * kv), F32)], axis=1))[:2 * kv]
    pe = sheet(x_all, 0, 8)[:, 2 * kv:]
    xe = early[:, :2 * kv]
    y = hdot(gc, xe, NT)
    xc = factor_inverse(gcc + eye - hdot(y, y, NT))
    x = jnp.concatenate([
        jnp.concatenate([xe, jnp.zeros((2 * kv, kv), F32)], axis=1),
        jnp.concatenate([-hdot(y, xe, NN), eye], axis=1)], axis=0)
    p = jnp.concatenate([
        jnp.concatenate([pe, pec], axis=1),
        jnp.concatenate([pc, pcc], axis=1)], axis=0)
    q = hdot(hdot(x, p, NN), x, NT)
    edge = lax.broadcasted_iota(jnp.int32, (2 * kv, 3 * kv), 0) == lax.broadcasted_iota(
        jnp.int32, (2 * kv, 3 * kv), 1)
    d = jnp.concatenate([
        jnp.where(edge, 1.0, 0.0).astype(F32),
        jnp.concatenate([jnp.zeros((kv, 2 * kv), F32), xc], axis=1)], axis=0)
    reduced[...] = hdot(hdot(d, q, NN), d, NT)
    drain(0, x_part, x_in)
    drain(1, y_part, y_in)
    result.wait()


def local(blocks, block_cols, live_counts, onsite_energy, precond, vectors, prev_vectors, prev_image):
    n = lax.axis_size("rows")
    br, slots, bs, _ = blocks.shape
    kv, width = vectors.shape
    nb = 3 * kv
    vmem = pl.BlockSpec(memory_space=pltpu.VMEM)
    smem = pl.BlockSpec(memory_space=pltpu.SMEM)
    hbm = pl.BlockSpec(memory_space=pl.ANY)
    dma = pltpu.SemaphoreType.DMA
    field = pltpu.VMEM((br, kv, bs), F32)
    halo = pltpu.VMEM((HB, kv, bs), F32)
    pair = pltpu.VMEM((br + HB + 1, 3 * kv, bs), BF16)
    moved = pltpu.VMEM((br, slots + 1, kv, bs), F32)

    def reduction(chunks):
        tiles = [(chunks, 8, 128), (n, 8, 128), (8, 128), (chunks, 8, 128)]
        return [pltpu.VMEM(t, F32) for t in tiles]

    return pl.pallas_call(
        functools.partial(kernel, n),
        out_shape=(
            jax.ShapeDtypeStruct((kv, width), F32),
            jax.ShapeDtypeStruct((nb, nb), F32),
        ),
        in_specs=[smem, smem, hbm, hbm, hbm, hbm, hbm, hbm],
        out_specs=(hbm, vmem),
        scratch_shapes=[
            pltpu.VMEM((br, bs, slots * bs), BF16),
            pltpu.VMEM((br, bs, slots * bs), E4M3),
            pltpu.VMEM((br, slots * bs, bs), BF16),
            pltpu.VMEM((br, slots * bs, bs), E4M3),
            pltpu.VMEM((br, bs, bs), BF16),
            pltpu.VMEM((br, bs, bs), BF16),
            pltpu.VMEM((RING, slots, bs, bs), F32),
            pltpu.VMEM((br, bs, bs), F32),
            pltpu.VMEM((1, width), F32),
            pltpu.VMEM((kv, width), F32),
            pltpu.VMEM((kv, width), F32),
            pltpu.VMEM((kv, width), F32),
            pltpu.VMEM((kv, width), F32),
            field, field, pair, pair, pair, moved, moved, moved, field, field, field,
            field, field, field, field, field, field,
            pltpu.VMEM((4, HB, kv, bs), F32),
            halo, halo,
            pltpu.VMEM((4, HB, kv, bs), F32),
            halo, halo, halo, halo, halo, halo,
            pltpu.VMEM((ROUNDS, 1, 128), F32),
            pltpu.VMEM((ROUNDS, n, 1, 128), F32),
            *reduction(24), *reduction(16),
            pltpu.VMEM((9, 1, 128), F32),
            pltpu.VMEM((n, 9, 1, 128), F32),
            pltpu.VMEM((2 * kv, 128), F32),
            dma((br,)),
            dma((4,)),
            dma((4,)),
            dma((1,)),
            dma((6,)),
            dma((6,)),
            dma((6,)),
            dma((6,)),
            dma((ROUNDS,)),
            dma((ROUNDS,)),
            dma((2,)),
            dma((2,)),
            dma((2,)),
            dma((2,)),
            dma((1,)),
            dma((1,)),
        ],
        compiler_params=pltpu.CompilerParams(
            collective_id=0, has_side_effects=True, vmem_limit_bytes=67043328
        ),
    )(block_cols.T, live_counts, blocks, precond, onsite_energy[None, :], vectors, prev_vectors, prev_image)


def solution(mesh):
    placed = (
        P("rows", None, None, None),
        P("rows", None),
        P("rows"),
        P("rows"),
        P("rows", None, None),
        P(None, "rows"),
        P(None, "rows"),
        P(None, "rows"),
    )
    return jax.shard_map(
        local, mesh=mesh, in_specs=placed, out_specs=(P(None, "rows"), P()), check_vma=False
    )
```

```python
import functools

import jax
import jax.numpy as jnp
from jax import lax
from jax.experimental import pallas as pl
from jax.experimental.pallas import tpu as pltpu
from jax.sharding import PartitionSpec as P

HB = 4
MESH = pl.DeviceIdType.MESH
F32 = jnp.float32
BF16 = jnp.bfloat16
E4M3 = jnp.float8_e4m3fn
NN = (((1,), (0,)), ((), ()))
NT = (((1,), (1,)), ((), ()))
LOW = 2.0 ** 20
RING = 8
ROUNDS = 3


def dot(a, b, dims):
    return lax.dot_general(a, b, dims, preferred_element_type=F32)


def hdot(a, b, dims):
    return lax.dot_general(a, b, dims, precision=lax.Precision.HIGHEST, preferred_element_type=F32)


def split(x):
    high = x.astype(BF16)
    low = (x - high.astype(F32)).astype(BF16)
    return high, low


def factor_inverse(s):
    m = s.shape[0]
    rows = lax.broadcasted_iota(jnp.int32, (m, 128), 0)
    lanes = lax.broadcasted_iota(jnp.int32, (m, m), 1)
    eye = jnp.where(lanes == lax.broadcasted_iota(jnp.int32, (m, m), 0), 1.0, 0.0).astype(F32)
    work = jnp.concatenate([s, eye, jnp.zeros((m, 128 - 2 * m), F32)], axis=1)
    diagonal = jnp.ones((m, 128), F32)
    for first in range(0, m, 8):
        column = [jnp.broadcast_to(work[:, first + i:first + i + 1], (m, 128)) for i in range(8)]
        for i in range(8):
            j = first + i
            pivot = column[i][j:j + 1]
            diagonal = jnp.where(rows == j, column[i], diagonal)
            below = jnp.where(rows > j, column[i] * (1.0 / pivot), 0.0)
            work = work - below * work[j:j + 1]
            for k in range(i + 1, 8):
                column[k] = column[k] - below * column[k][j:j + 1]
    return (work / jnp.sqrt(diagonal))[:, m:2 * m]


def kernel(
    n, cols, counts, blocks, precond, onsite_hbm, vectors_hbm, prev_vectors_hbm, prev_image_hbm,
    correction, reduced,
    w_high, w_low, t_high, t_low, m_high, m_low, stage, pstage,
    onsite, vec, pvec, pimg, cor,
    field, fieldv, pair, pairv, pairp, moved, movedv, movedp, fwd, fwdv, fwdp,
    image, rem, app, srch, hsrch, hturn,
    halo_in, halov_in, land_out, land_in, landv_out, landv_in, p_out, p_in, landp_out, landp_in,
    part, sums_in, x_part, x_in, x_sum, x_all, y_part, y_in, y_sum, y_all,
    f_part, f_in, early,
    load_sem, pload_sem, in_sem, out_sem, halo_send, halo_recv, land_send, land_recv,
    sum_send, sum_recv, r_send, r_recv, a_send, a_recv, f_send, f_recv,
):
    me = lax.axis_index("rows")
    right, left = lax.rem(me + 1, n), lax.rem(me + n - 1, n)
    br, slots, bs = blocks.shape[0], blocks.shape[1], blocks.shape[2]
    kv = 32
    total = br * n
    first = br - HB
    order = list(range(first, br)) + list(range(first))
    pchunk = br // 4

    def lanes(b):
        return pl.ds(b * bs, bs)

    def load(t):
        return pltpu.make_async_copy(blocks.at[order[t]], stage.at[t % RING], load_sem.at[t])

    def pload(c):
        at = pl.ds(c * pchunk, pchunk)
        return pltpu.make_async_copy(precond.at[at], pstage.at[at], pload_sem.at[c])

    inputs = [
        pltpu.make_async_copy(vectors_hbm, vec, in_sem.at[0]),
        pltpu.make_async_copy(onsite_hbm, onsite, in_sem.at[1]),
        pltpu.make_async_copy(prev_vectors_hbm, pvec, in_sem.at[2]),
        pltpu.make_async_copy(prev_image_hbm, pimg, in_sem.at[3]),
    ]
    barrier = pltpu.get_barrier_semaphore()
    inputs[0].start()
    inputs[1].start()
    for t in range(RING):
        load(t).start()
    for c in range(4):
        pload(c).start()
    inputs[2].start()
    inputs[3].start()

    def greet(d, _):
        pl.semaphore_signal(barrier, inc=1, device_id=(lax.rem(me + d, n),), device_id_type=MESH)
        return 0

    lax.fori_loop(1, n, greet, 0)

    def offset(b, s):
        return lax.rem(cols[s, b] - (me * br + b) + total, total)

    def source(b, s):
        return jnp.where(s < counts[b], b + offset(b, s), br + HB)

    def slot_of(b, k):
        at = jnp.int32(slots)
        for s in range(slots):
            at = jnp.where((s < counts[b]) & (offset(b, s) == k), s, at)
        return at

    def put(to, b, x):
        high = x.astype(BF16)
        wide = high.astype(F32)
        to[b, 0:kv] = high
        to[b, kv:2 * kv] = (x - wide).astype(BF16)
        to[b, 2 * kv:3 * kv] = (wide * (1.0 / LOW)).astype(BF16)

    def take_tiles(t):
        b = order[t]
        for s in range(slots):
            at = slice(s * bs, (s + 1) * bs)
            x = stage[t % RING, s]
            high = x.astype(BF16)
            low = ((x - high.astype(F32)) * LOW).astype(E4M3)
            w_high[b, :, at] = high
            w_low[b, :, at] = low
            t_high[b, at, :] = high.T
            t_low[b, at, :] = low.T

    def spread(b, groups):
        lhs = jnp.concatenate([g[0][b, 0:2 * kv] for g in groups], axis=0)
        out = dot(lhs, w_high[b], NN)
        low = dot(jnp.concatenate([g[0][b, 2 * kv:3 * kv] for g in groups], axis=0), w_low[b], NN)
        for i, g in enumerate(groups):
            whole = out[2 * i * kv:(2 * i + 1) * kv] + out[(2 * i + 1) * kv:(2 * i + 2) * kv] + low[i * kv:(i + 1) * kv]
            for s in range(slots):
                g[1][b, s] = whole[:, s * bs:(s + 1) * bs]

    def forward(b, groups):
        at = [source(b, s) for s in range(slots)]
        lhs = jnp.concatenate(
            [jnp.concatenate([g[0][a, 0:2 * kv] for a in at], axis=1) for g in groups], axis=0)
        lhs_low = jnp.concatenate(
            [jnp.concatenate([g[0][a, 2 * kv:3 * kv] for a in at], axis=1) for g in groups], axis=0)
        out = dot(lhs, t_high[b], NN)
        low = dot(lhs_low, t_low[b], NN)
        for i, g in enumerate(groups):
            g[2][b] = out[2 * i * kv:(2 * i + 1) * kv] + out[(2 * i + 1) * kv:(2 * i + 2) * kv] + low[i * kv:(i + 1) * kv]

    def landing(group, b):
        got = None
        for k in range(HB + 1):
            c = b - k
            if 0 <= c < br:
                one = group[1][c, slot_of(c, k)]
                got = one if got is None else got + one
        return got

    def halo_copy(k, src, dst):
        return pltpu.make_async_remote_copy(
            src_ref=src.at[pl.ds(0, HB)], dst_ref=dst,
            send_sem=halo_send.at[k], recv_sem=halo_recv.at[k],
            device_id=(left,), device_id_type=MESH)

    def land_copy(k, src, dst):
        return pltpu.make_async_remote_copy(
            src_ref=src, dst_ref=dst,
            send_sem=land_send.at[k], recv_sem=land_recv.at[k],
            device_id=(right,), device_id_type=MESH)

    main = (pair, moved, fwd)
    side = (pairv, movedv, fwdv)
    rear = (pairp, movedp, fwdp)

    def blockloop(lo, hi, body, unroll):
        def step(b, _):
            body(b)
            return 0

        lax.fori_loop(lo, hi, step, 0, unroll=unroll)

    def precondition(b, x):
        high, low = split(x)
        both = dot(jnp.concatenate([high, low], axis=0), m_high[b], NN)
        return both[:kv] + both[kv:] + dot(high, m_low[b], NN)

    def every(lo, hi, body):
        if hi - lo <= 32:
            for d in range(lo, hi):
                body(d)
        else:
            def step(d, _):
                body(d)
                return 0

            lax.fori_loop(lo, hi, step, 0)

    def sum_copy(k, d):
        return pltpu.make_async_remote_copy(
            src_ref=part.at[k], dst_ref=sums_in.at[k, me],
            send_sem=sum_send.at[k], recv_sem=sum_recv.at[k],
            device_id=(lax.rem(me + d, n),), device_id_type=MESH)

    def lane_sums(one, two):
        folded = jnp.concatenate([one, two], axis=0)
        folded = folded[:, :128] + folded[:, 128:]
        return jnp.sum(folded, axis=1, keepdims=True)

    def sum_start(k, one, two):
        wide = jnp.broadcast_to(lane_sums(one, two), (2 * kv, 128))
        wide = jnp.concatenate([wide, jnp.zeros((128 - 2 * kv, 128), F32)], axis=0)
        mine = wide.T[:1]
        part[k] = mine
        sums_in[k, me] = mine

        every(1, n, lambda d: sum_copy(k, d).start())

    def bulk(ref, sem):
        return pltpu.make_async_copy(ref, ref, sem)

    def sum_finish(k):
        bulk(sums_in.at[k, pl.ds(0, n - 1)], sum_recv.at[k]).wait()
        whole = jnp.sum(sums_in[k], axis=0)
        bulk(sums_in.at[k, pl.ds(0, n - 1)], sum_send.at[k]).wait()
        column = jnp.broadcast_to(whole, (128, 128)).T
        column = jnp.concatenate([column, column], axis=1)
        return column[:kv], column[kv:2 * kv]

    def scatter(r, sheet, held, landed):
        chunks = held.shape[0]
        for c in range(chunks):
            if sheet[c] is not None:
                held[c] = sheet[c]

        def send(d):
            to = lax.rem(me + d, chunks)

            @pl.when(to != me)
            def _():
                pltpu.make_async_remote_copy(
                    src_ref=held.at[to], dst_ref=landed.at[me],
                    send_sem=r_send.at[r], recv_sem=r_recv.at[r],
                    device_id=(to,), device_id_type=MESH).start()

        every(0, chunks, send)

    def spread_sums(r, held, landed, mine, everything):
        chunks = held.shape[0]

        @pl.when(me < chunks)
        def _():
            bulk(landed.at[pl.ds(0, n - 1)], r_recv.at[r]).wait()
            landed[me] = held[jnp.minimum(me, chunks - 1)]
            whole = jnp.sum(landed[...], axis=0)
            mine[...] = whole
            everything[jnp.minimum(me, chunks - 1)] = whole

            def send(d):
                pltpu.make_async_remote_copy(
                    src_ref=mine, dst_ref=everything.at[jnp.minimum(me, chunks - 1)],
                    send_sem=a_send.at[r], recv_sem=a_recv.at[r],
                    device_id=(lax.rem(me + d, n),), device_id_type=MESH).start()

            every(1, n, send)

    def collect(r, held, landed, everything):
        chunks = held.shape[0]

        @pl.when(me < chunks)
        def _():
            bulk(everything.at[pl.ds(0, chunks - 1)], a_recv.at[r]).wait()

        @pl.when(me >= chunks)
        def _():
            bulk(everything, a_recv.at[r]).wait()

    def drain(r, held, landed):
        chunks = held.shape[0]

        @pl.when(me < chunks)
        def _():
            bulk(held.at[pl.ds(0, chunks - 1)], r_send.at[r]).wait()
            bulk(landed.at[pl.ds(0, n - 1)], a_send.at[r]).wait()

        @pl.when(me >= chunks)
        def _():
            bulk(held, r_send.at[r]).wait()

    zero = jnp.zeros((kv, bs), F32)
    for c in range(br):
        moved[c, slots] = zero
        movedv[c, slots] = zero
        movedp[c, slots] = zero
    pair[br + HB] = jnp.zeros((3 * kv, bs), BF16)
    pairv[br + HB] = jnp.zeros((3 * kv, bs), BF16)
    pairp[br + HB] = jnp.zeros((3 * kv, bs), BF16)
    inputs[0].wait()
    for b in range(br):
        x = vec[:, lanes(b)]
        put(pair, b, x)
        if b < HB:
            field[b] = x

    def advance(t):
        load(t).wait()
        if t and t - 1 + RING < br:
            load(t - 1 + RING).start()

    for t in range(HB):
        advance(t)
        if t:
            spread(order[t - 1], [main])
        take_tiles(t)
    spread(order[HB - 1], [main])
    for i in range(HB):
        land_out[i] = landing(main, br + i)
    pl.semaphore_wait(barrier, n - 1)
    halo = halo_copy(0, field, halo_in.at[0])
    halo.start()
    land = land_copy(0, land_out, land_in.at[0])
    land.start()
    for t in range(HB, br):
        advance(t)
        if t > HB:
            spread(order[t - 1], [main])
            forward(order[t - 1], [main])
        take_tiles(t)
    spread(first - 1, [main])
    forward(first - 1, [main])

    for c in range(4):
        pload(c).wait()
    for b in range(br):
        high, low = split(pstage[b])
        m_high[b] = high.T
        m_low[b] = low.T

    def side_block(b):
        x = precondition(b, vec[:, lanes(b)])
        fieldv[b] = x
        put(pairv, b, x)

    for b in list(range(HB)) + list(range(first, br)):
        side_block(b)
    halov = halo_copy(4, fieldv, halov_in)
    halov.start()
    for b in range(first, br):
        spread(b, [side])
    for i in range(HB):
        landv_out[i] = landing(side, br + i)
    landv = land_copy(4, landv_out, landv_in)
    landv.start()
    for b in range(HB, first):
        side_block(b)

    inputs[1].wait()

    def finish(k, groups, halo, land, more):
        halo.wait_recv()
        for i in range(HB):
            put(pair, br + i, halo_in[k, i])
        for group, copies, arrived in more:
            copies[0].wait_recv()
            for i in range(HB):
                put(group[0], br + i, arrived[i])
        for b in range(first, br):
            forward(b, groups)
        land.wait_recv()
        for group, copies, arrived in more:
            copies[1].wait_recv()
            copies[0].wait_send()
            copies[1].wait_send()
        halo.wait_send()
        land.wait_send()

    def begin(k, update, outs_to, send_sums):
        def pre(b, x):
            y = precondition(b, x)
            outs_to[b] = y
            put(pair, b, y)

        for b in range(HB):
            pre(b, update(b))
        halo = halo_copy(k, outs_to, halo_in.at[k])
        halo.start()
        outs = [update(b) for b in range(first, br)]
        for b in range(first, br):
            pre(b, outs[b - first])
        outs = [update(b) for b in range(HB, first)]
        send_sums()
        for b in range(first, br):
            spread(b, [main])
        for i in range(HB):
            land_out[i] = landing(main, br + i)
        land = land_copy(k, land_out, land_in.at[k])
        land.start()

        def rest():
            for b in range(HB, first):
                pre(b, outs[b - HB])

        return halo, land, rest

    def middle(groups):
        def both_ways(b):
            spread(b, groups)
            forward(b, groups)

        blockloop(0, first, both_ways, 4)

    def totals():
        sums = [zero, zero]

        def add(a, c):
            sums[0] = sums[0] + a
            sums[1] = sums[1] + c

        return sums, add

    def gram(lhs, rhs):
        got = None
        for b in range(br):
            lh, ll = split(jnp.concatenate(lhs(b), axis=0))
            rh, rl = split(jnp.concatenate(rhs(b), axis=0))
            m = lh.shape[0]
            both = dot(jnp.concatenate([lh, ll], axis=0), rh, NT)
            one = both[:m] + both[m:] + dot(lh, rl, NT)
            got = one if got is None else got + one
        return got

    def rows8(sheets):
        return [s[c * 8:(c + 1) * 8] for s in sheets for c in range(s.shape[0] // 8)]

    finish(0, [main], halo, land, ())

    sums, add = totals()

    def after0(b):
        x = vec[:, lanes(b)]
        got = fwd[b] + landing(main, b) + onsite[:, lanes(b)] * x
        if b < HB:
            got = got + land_in[0, b]
        image[b] = got
        add(x * got, x * x)
        return got

    halo, land, rest = begin(1, after0, field, lambda: sum_start(0, *sums))
    rest()
    middle([main, side])
    inputs[2].wait()
    inputs[3].wait()
    for b in range(br):
        x = pvec[:, lanes(b)]
        put(pairp, b, x)
        if b < HB:
            p_out[b] = x
    halop = halo_copy(5, p_out, p_in)
    halop.start()
    for b in range(first, br):
        spread(b, [rear])
    for i in range(HB):
        landp_out[i] = landing(rear, br + i)
    landp = land_copy(5, landp_out, landp_in)
    landp.start()
    both = gram(lambda b: [vec[:, lanes(b)], pvec[:, lanes(b)]],
                lambda b: [vec[:, lanes(b)], pvec[:, lanes(b)], image[b], pimg[:, lanes(b)]])
    for c, rows in enumerate(rows8([both])):
        x_part[c] = rows
    finish(1, [main, side], halo, land, [(side, (halov, landv), halov_in)])
    numerator, denominator = sum_finish(0)
    quotient = numerator / denominator

    sums, add = totals()

    def after1(b):
        xv, xi = fieldv[b], field[b]
        on = onsite[:, lanes(b)]
        hv = fwdv[b] + landing(side, b) + on * xv
        hi = fwd[b] + landing(main, b) + on * xi
        if b < HB:
            hv = hv + landv_in[b]
            hi = hi + land_in[1, b]
        x = quotient * xv - xi
        h = quotient * hv - hi
        r = quotient * vec[:, lanes(b)] - image[b]
        a = h - quotient * x
        srch[b] = x
        hsrch[b] = h
        rem[b] = r
        app[b] = a
        add(a * r, a * a)
        return a

    halo, land, rest = begin(2, after1, field, lambda: sum_start(1, *sums))
    rest()
    middle([main, rear])
    both = gram(lambda b: [srch[b], field[b]],
                lambda b: [vec[:, lanes(b)], pvec[:, lanes(b)], srch[b], field[b],
                           image[b], pimg[:, lanes(b)], hsrch[b], hsrch[b]])
    scatter(0, [None] * 8 + rows8([both[:, :128], both[:, 128:]]), x_part, x_in)
    finish(2, [main, rear], halo, land, [(rear, (halop, landp), p_in)])

    def after2(b):
        t = field[b]
        got = fwd[b] + landing(main, b) + onsite[:, lanes(b)] * t
        if b < HB:
            got = got + land_in[2, b]
        hturn[b] = got
        return got - quotient * t

    halo, land, rest = begin(3, after2, fieldv, lambda: None)
    step = sum_finish(1)
    step1 = step[0] / (step[1] + 1.0)
    sums, add = totals()
    for b in range(br):
        r = rem[b] - step1 * app[b]
        a = app[b] - step1 * (hturn[b] - quotient * field[b])
        rem[b] = r
        app[b] = a
        add(a * r, a * a)
    sum_start(2, *sums)
    rest()
    for b in range(br):
        got = fwdp[b] + landing(rear, b) + onsite[:, lanes(b)] * pvec[:, lanes(b)]
        fwdp[b] = got + landp_in[b] if b < HB else got
    one = gram(lambda b: [fieldv[b]],
               lambda b: [vec[:, lanes(b)], pvec[:, lanes(b)], srch[b], field[b],
                          image[b], pimg[:, lanes(b)], hsrch[b], fieldv[b]])
    two = gram(lambda b: [fieldv[b], srch[b], field[b]], lambda b: [fwdp[b], hturn[b]])
    three = jnp.concatenate([two[:kv], two[2 * kv:]], axis=1)
    four = jnp.concatenate([two[kv:2 * kv], two[kv:2 * kv]], axis=1)
    scatter(1, rows8([one[:, :128], one[:, 128:], three, four]), y_part, y_in)
    middle([main])
    spread_sums(0, x_part, x_in, x_sum, x_all)
    finish(3, [main], halo, land, ())
    spread_sums(1, y_part, y_in, y_sum, y_all)
    step = sum_finish(2)
    step2 = step[0] / (step[1] + 1.0)

    sums, add = totals()
    for b in range(br):
        u = fieldv[b]
        got = fwd[b] + landing(main, b) + onsite[:, lanes(b)] * u
        if b < HB:
            got = got + land_in[3, b]
        image[b] = got
        a = app[b]
        r = rem[b] - step2 * a
        g = hturn[b] - quotient * field[b]
        a = a - step2 * (g - step1 * (got - quotient * u))
        add(a * r, a * a)
    square = gram(lambda b: [fieldv[b]], lambda b: [image[b]])
    flat = jnp.concatenate([square[8 * c:8 * c + 8] for c in range(4)], axis=1)
    wide = jnp.broadcast_to(lane_sums(*sums), (2 * kv, 128))
    wide = jnp.concatenate([wide, jnp.zeros((128 - 2 * kv, 128), F32)], axis=0)
    f_part[8] = wide.T[:1]
    for i in range(8):
        f_part[i] = flat[i:i + 1]
    f_in[me] = f_part[...]

    def last_send(d):
        pltpu.make_async_remote_copy(
            src_ref=f_part, dst_ref=f_in.at[me],
            send_sem=f_send.at[0], recv_sem=f_recv.at[0],
            device_id=(lax.rem(me + d, n),), device_id_type=MESH).start()

    every(1, n, last_send)


    collect(0, x_part, x_in, x_all)
    known = jnp.concatenate([x_all[c] for c in range(8)], axis=0)
    rows_at = lax.broadcasted_iota(jnp.int32, (kv, kv), 0)
    eye = jnp.where(rows_at == lax.broadcasted_iota(jnp.int32, (kv, kv), 1), 1.0, 0.0).astype(F32)
    x11 = factor_inverse(known[:kv, :kv] + eye)
    y21 = hdot(known[kv:2 * kv, :kv], x11, NT)
    x22 = factor_inverse(known[kv:2 * kv, kv:2 * kv] + eye - hdot(y21, y21, NT))
    x21 = -hdot(x22, hdot(y21, x11, NN), NN)
    early[0:kv] = jnp.concatenate([x11, jnp.zeros((kv, 128 - kv), F32)], axis=1)
    early[kv:2 * kv] = jnp.concatenate([x21, x22, jnp.zeros((kv, 128 - 2 * kv), F32)], axis=1)
    collect(1, y_part, y_in, y_all)

    def sheet(held, i, count):
        return jnp.concatenate([held[i * count + c] for c in range(count)], axis=0)

    def turned(t):
        return jnp.concatenate([t, jnp.zeros((128 - kv, 128), F32)], axis=0).T[:, :kv]

    xg, xh = sheet(x_all, 1, 8), sheet(x_all, 2, 8)
    ug, uh, third, fourth = [sheet(y_all, i, 4) for i in range(4)]
    ug_t, uh_t, third_t = turned(ug), turned(uh), turned(third)
    bulk(f_in.at[pl.ds(0, n - 1)], f_recv.at[0]).wait()
    whole = jnp.sum(f_in[...], axis=0)
    bulk(f_in.at[pl.ds(0, n - 1)], f_send.at[0]).wait()
    flat = jnp.concatenate([whole[i] for i in range(8)], axis=0)
    uhu = jnp.concatenate([flat[:, kv * c:kv * c + kv] for c in range(4)], axis=0)
    column = jnp.broadcast_to(whole[8], (128, 128)).T
    step3 = column[:kv] / (column[kv:2 * kv] + 1.0)
    step1, step2 = step1[:, :128], step2[:, :128]
    ca = step1 + step2 + step3
    ct = -(step1 * step2 + step3 * (step1 + step2))
    cu = step1 * step2 * step3
    wa, wt, wu = [jnp.concatenate([c, c], axis=1) for c in (ca, ct, cu)]
    for b in range(br):
        cor[:, lanes(b)] = wa * srch[b] + wt * field[b] + wu * fieldv[b]
    result = pltpu.make_async_copy(cor, correction, out_sem.at[0])
    result.start()
    row = jnp.concatenate([ca, ct, cu, jnp.zeros((128 - 3 * kv, 128), F32)], axis=0).T
    ra, rt, ru = [row[:kv, kv * i:kv * i + kv] for i in range(3)]
    g = ca * xg[:kv] + ct * xg[kv:] + cu * ug
    h = ca * xh[:kv] + ct * xh[kv:] + cu * uh
    na, nt, nu = ca[:, :kv], ct[:, :kv], cu[:, :kv]
    gu = na * ug_t[2 * kv:3 * kv] + nt * ug_t[3 * kv:] + nu * uh[:, 3 * kv:]
    gc = g[:, :2 * kv]
    gcc = g[:, 2 * kv:3 * kv] * ra + g[:, 3 * kv:] * rt + gu * ru
    pc = h[:, :2 * kv]
    both = ca * jnp.concatenate([fourth[:, :2 * kv], fourth[:, :2 * kv]], axis=1) + cu * third
    chp = both[:, :kv] + nt * third[:, 2 * kv:3 * kv]
    cht = both[:, kv:2 * kv] + nt * third[:, 3 * kv:]
    chu = na * uh_t[2 * kv:3 * kv] + nt * third_t[kv:2 * kv] + nu * uhu
    pcc = h[:, 2 * kv:3 * kv] * ra + cht * rt + chu * ru
    pec = turned(jnp.concatenate([h[:, :kv], chp, jnp.zeros((kv, 128 - 2 * kv), F32)], axis=1))[:2 * kv]
    pe = sheet(x_all, 0, 8)[:, 2 * kv:]
    xe = early[:, :2 * kv]
    y = hdot(gc, xe, NT)
    xc = factor_inverse(gcc + eye - hdot(y, y, NT))
    x = jnp.concatenate([
        jnp.concatenate([xe, jnp.zeros((2 * kv, kv), F32)], axis=1),
        jnp.concatenate([-hdot(y, xe, NN), eye], axis=1)], axis=0)
    p = jnp.concatenate([
        jnp.concatenate([pe, pec], axis=1),
        jnp.concatenate([pc, pcc], axis=1)], axis=0)
    q = hdot(hdot(x, p, NN), x, NT)
    edge = lax.broadcasted_iota(jnp.int32, (2 * kv, 3 * kv), 0) == lax.broadcasted_iota(
        jnp.int32, (2 * kv, 3 * kv), 1)
    d = jnp.concatenate([
        jnp.where(edge, 1.0, 0.0).astype(F32),
        jnp.concatenate([jnp.zeros((kv, 2 * kv), F32), xc], axis=1)], axis=0)
    reduced[...] = hdot(hdot(d, q, NN), d, NT)
    drain(0, x_part, x_in)
    drain(1, y_part, y_in)
    result.wait()


def local(blocks, block_cols, live_counts, onsite_energy, precond, vectors, prev_vectors, prev_image):
    n = lax.axis_size("rows")
    br, slots, bs, _ = blocks.shape
    kv, width = vectors.shape
    nb = 3 * kv
    vmem = pl.BlockSpec(memory_space=pltpu.VMEM)
    smem = pl.BlockSpec(memory_space=pltpu.SMEM)
    hbm = pl.BlockSpec(memory_space=pl.ANY)
    dma = pltpu.SemaphoreType.DMA
    field = pltpu.VMEM((br, kv, bs), F32)
    halo = pltpu.VMEM((HB, kv, bs), F32)
    pair = pltpu.VMEM((br + HB + 1, 3 * kv, bs), BF16)
    moved = pltpu.VMEM((br, slots + 1, kv, bs), F32)

    def reduction(chunks):
        tiles = [(chunks, 8, 128), (n, 8, 128), (8, 128), (chunks, 8, 128)]
        return [pltpu.VMEM(t, F32) for t in tiles]

    return pl.pallas_call(
        functools.partial(kernel, n),
        out_shape=(
            jax.ShapeDtypeStruct((kv, width), F32),
            jax.ShapeDtypeStruct((nb, nb), F32),
        ),
        in_specs=[smem, smem, hbm, hbm, hbm, hbm, hbm, hbm],
        out_specs=(hbm, vmem),
        scratch_shapes=[
            pltpu.VMEM((br, bs, slots * bs), BF16),
            pltpu.VMEM((br, bs, slots * bs), E4M3),
            pltpu.VMEM((br, slots * bs, bs), BF16),
            pltpu.VMEM((br, slots * bs, bs), E4M3),
            pltpu.VMEM((br, bs, bs), BF16),
            pltpu.VMEM((br, bs, bs), BF16),
            pltpu.VMEM((RING, slots, bs, bs), F32),
            pltpu.VMEM((br, bs, bs), F32),
            pltpu.VMEM((1, width), F32),
            pltpu.VMEM((kv, width), F32),
            pltpu.VMEM((kv, width), F32),
            pltpu.VMEM((kv, width), F32),
            pltpu.VMEM((kv, width), F32),
            field, field, pair, pair, pair, moved, moved, moved, field, field, field,
            field, field, field, field, field, field,
            pltpu.VMEM((4, HB, kv, bs), F32),
            halo, halo,
            pltpu.VMEM((4, HB, kv, bs), F32),
            halo, halo, halo, halo, halo, halo,
            pltpu.VMEM((ROUNDS, 1, 128), F32),
            pltpu.VMEM((ROUNDS, n, 1, 128), F32),
            *reduction(24), *reduction(16),
            pltpu.VMEM((9, 1, 128), F32),
            pltpu.VMEM((n, 9, 1, 128), F32),
            pltpu.VMEM((2 * kv, 128), F32),
            dma((br,)),
            dma((4,)),
            dma((4,)),
            dma((1,)),
            dma((6,)),
            dma((6,)),
            dma((6,)),
            dma((6,)),
            dma((ROUNDS,)),
            dma((ROUNDS,)),
            dma((2,)),
            dma((2,)),
            dma((2,)),
            dma((2,)),
            dma((1,)),
            dma((1,)),
        ],
        compiler_params=pltpu.CompilerParams(
            collective_id=0, has_side_effects=True, vmem_limit_bytes=67043328
        ),
    )(block_cols.T, live_counts, blocks, precond, onsite_energy[None, :], vectors, prev_vectors, prev_image)


def solution(mesh):
    placed = (
        P("rows", None, None, None),
        P("rows", None),
        P("rows"),
        P("rows"),
        P("rows", None, None),
        P(None, "rows"),
        P(None, "rows"),
        P(None, "rows"),
    )
    return jax.shard_map(
        local, mesh=mesh, in_specs=placed, out_specs=(P(None, "rows"), P()), check_vma=False
    )
```
